256 devices in a mesh: section: 2 (over core), seq: 128 (over x, z, y).
Axes of the slice: x: 4, y: 4, z: 8, core: 2. Of those that a mesh axis runs over, the one named last changes fastest.
Arguments:
- acts: bfloat16 [2, 32768, 2048], P('section', 'seq'), may hold values from -6 to 6
- in_proj: bfloat16 [2, 2048, 4640], P('section', 'seq'), may hold values from -0.125 to 0.125
- out_proj: bfloat16 [2, 2048, 2048], P('section'), may hold values from -0.125 to 0.125
- conv_weight: float32 [2, 4, 2304], P('section'), may hold values from -3 to 3
- conv_bias: float32 [2, 2304], P('section'), may hold values from -3 to 3
- dt_bias: float32 [2, 32], P('section'), may hold values from -4 to -1
- decay_rate: float32 [2, 32], P('section'), may hold values from 0.0001 to 0.5
- skip_gain: float32 [2, 32], P('section'), may hold values from -4 to 4
- level_bias: float32 [2, 256], P('section'), may hold values from -4 to 4
- norm_gain: float32 [2, 2048], P('section'), may hold values from 0.5 to 1.5
- gate_gain: float32 [2, 2048], P('section'), may hold values from 0.5 to 1.5
Outputs:
- handoff: bfloat16 [2, 32768, 2048], P('section', 'seq')
The draws below stay inside these ranges and needn't reach their ends.
All inputs are finite; a program needn't handle non-finite values.
Results may differ from the reference program's by a relative error of at most 0.006.
Values may be sent and summed in bfloat16 or wider, within the bound.
No kernel may reach another device: no remote copies, remote signals or barrier semaphores. Data moves between devices by JAX's collectives and lax.ppermute only.
A program may use at most 128 MiB of HBM per device.

```python
import math
import jax
import jax.numpy as jnp
from jax import lax

D = 2048
CONV = 4
HEADS = 32
LEVELS = 8
SECTIONS = 2
DI = 2048
CH = 2304
PROJ = 4640
SEQLEN = 32768
N_SEQ = 128


def block_levels(key, extent, shards, low, largest):
    loudness = 1.0
    for axis_at, parts in shards:
        steps = jax.random.uniform(jax.random.fold_in(jax.random.fold_in(key, 6), axis_at), (parts,), jnp.float32, low / len(shards), largest / len(shards))
        loudness = loudness * jnp.repeat(jnp.exp(steps), extent[axis_at] // parts).reshape((-1,) + (1,) * (len(extent) - 1 - axis_at))
    return loudness


def normal_values(key, extent, width, reach, pieces=(), kind=jnp.bfloat16):
    loudness = block_levels(key, extent, pieces, -0.22, 0.18) if pieces else 1.0
    values = jax.random.normal(key, extent, jnp.float32) * width * loudness
    return jnp.minimum(jnp.maximum(values, -reach), reach).astype(kind)


def setup_inputs(seed: int = 0) -> dict:
    streams_of = jax.random.split(jax.random.key(seed), 12)
    acts = normal_values(streams_of[0], (SECTIONS, SEQLEN, D), 1.0, 6.0, ((0, 2), (1, 128)))
    in_proj = normal_values(streams_of[1], (SECTIONS, D, PROJ), D ** -0.5, 0.125, ((0, 2), (1, 128)))
    out_proj = normal_values(streams_of[2], (SECTIONS, DI, D), DI ** -0.5, 0.125, ((0, 2),))
    conv_weight = normal_values(streams_of[3], (SECTIONS, CONV, CH), 0.6, 3.0, ((0, 2),), jnp.float32)
    conv_bias = normal_values(streams_of[4], (SECTIONS, CH), 0.5, 3.0, ((0, 2),), jnp.float32)
    dt_bias = jnp.clip(-4.0 + 3.0 * jax.random.uniform(streams_of[5], (SECTIONS, HEADS), jnp.float32) ** block_levels(streams_of[5], (SECTIONS, HEADS), ((0, 2),), -0.2, 0.2), -4.0, -1.0)
    decay_rate = jnp.clip(jnp.exp(math.log(0.5) - 8.517193 * jax.random.uniform(streams_of[6], (SECTIONS, HEADS), jnp.float32) ** block_levels(streams_of[6], (SECTIONS, HEADS), ((0, 2),), -0.2, 0.2)), 0.0001, 0.5)
    skip_gain = normal_values(streams_of[7], (SECTIONS, HEADS), 1.0, 4.0, ((0, 2),), jnp.float32)
    level_bias = normal_values(streams_of[8], (SECTIONS, HEADS * LEVELS), 1.0, 4.0, ((0, 2),), jnp.float32)
    norm_gain = jnp.clip(1.0 + 0.1 * jax.random.normal(streams_of[9], (SECTIONS, D), jnp.float32), 0.5, 1.5)
    gate_gain = jnp.clip(1.0 + 0.1 * jax.random.normal(streams_of[10], (SECTIONS, DI), jnp.float32), 0.5, 1.5)
    return dict(acts=acts, in_proj=in_proj, out_proj=out_proj, conv_weight=conv_weight, conv_bias=conv_bias, dt_bias=dt_bias, decay_rate=decay_rate, skip_gain=skip_gain, level_bias=level_bias, norm_gain=norm_gain, gate_gain=gate_gain)


EPS = 1e-05
best_precision = lax.Precision.HIGHEST

def block_core(operands):
    c_block, b_block, x_block, cum_block, dt_block, lam_block = operands
    length = c_block.shape[0]
    scores = jnp.dot(c_block, b_block.T, precision=best_precision, preferred_element_type=jnp.float32)
    row_ids = lax.broadcasted_iota(jnp.int32, (length, length), 0)
    col_ids = lax.broadcasted_iota(jnp.int32, (length, length), 1)
    causal = (col_ids <= row_ids)[:, :, None]
    differ = cum_block[:, None, :] - cum_block[None, :, :]
    decays = jnp.where(causal, jnp.exp(jnp.where(causal, differ, 0.0)), 0.0)
    weights = decays * scores[:, :, None] * dt_block[None, :, :] * lam_block[:, None, :]
    y_block = jnp.einsum('tsh,shp->thp', weights, x_block, precision=best_precision)
    tail = jnp.exp(cum_block[-1][None, :] - cum_block) * dt_block
    state = jnp.einsum('sn,shp->hnp', b_block, x_block * tail[:, :, None], precision=best_precision)
    return (y_block, state)

def mixer(acts, w_in, w_out, conv_w, conv_b, dt_b, rate, skip, lam_b, gain_in, gain_gate):
    hidden = acts.astype(jnp.float32)
    seqlen = hidden.shape[0]
    inner = gain_gate.shape[0]
    heads = dt_b.shape[0]
    head_size = inner // heads
    chans = conv_w.shape[1]
    state_size = (chans - inner) // 2
    kernel_len = conv_w.shape[0]
    normed_in = (hidden * lax.rsqrt(lax.optimization_barrier(jnp.mean(hidden * hidden, axis=1, keepdims=True)) + EPS) * gain_in).astype(jnp.bfloat16)
    projected = jnp.dot(normed_in, w_in, preferred_element_type=jnp.float32).astype(jnp.bfloat16)
    conv_in = jnp.concatenate([jnp.zeros((kernel_len - 1, chans), jnp.float32), projected[:, :chans].astype(jnp.float32)], axis=0)
    mixed = conv_b + jnp.zeros((seqlen, chans), jnp.float32)
    for offset in range(kernel_len):
        mixed = mixed + conv_w[offset] * conv_in[offset:offset + seqlen]
    mixed = jax.nn.silu(mixed)
    values = mixed[:, :inner].reshape(seqlen, heads, head_size)
    b_mat = mixed[:, inner:inner + state_size]
    c_mat = mixed[:, inner + state_size:]
    z_gate = projected[:, chans:chans + inner].astype(jnp.float32)
    steps = jax.nn.softplus(projected[:, chans + inner:chans + inner + heads].astype(jnp.float32) + dt_b)
    lam = jax.nn.softplus(projected[:, chans + inner + heads:].astype(jnp.float32) + lam_b).reshape(seqlen, heads, LEVELS)
    blocks = N_SEQ
    length = seqlen // blocks
    log_decay = (-steps * rate).reshape(blocks, length, heads)
    cum = jnp.cumsum(log_decay, axis=1)
    x_blocks = values.reshape(blocks, length, heads, head_size)
    b_blocks = b_mat.reshape(blocks, length, state_size)
    c_blocks = c_mat.reshape(blocks, length, state_size)
    dt_blocks = steps.reshape(blocks, length, heads)
    lam_blocks = lam.reshape(blocks, length, heads, LEVELS)
    y_all, states = lax.map(block_core, (c_blocks, b_blocks, x_blocks, cum, dt_blocks, lam_blocks[..., 0]))
    y_all = y_all + skip[None, None, :, None] * x_blocks
    endlog = cum[:, -1, :]
    inclusive = jnp.cumsum(endlog, axis=0)
    exclusive = inclusive - endlog
    for level in range(1, blocks.bit_length()):
        half = 2 ** (level - 1)
        groups = blocks // (2 * half)
        lower_states = states.reshape(groups, 2, half, heads, state_size, head_size)[:, 0]
        incl_groups = inclusive.reshape(groups, 2, half, heads)
        lower_end = incl_groups[:, 0, half - 1]
        weights = jnp.exp(lower_end[:, None, :] - incl_groups[:, 0])
        summed = jnp.einsum('gjh,gjhnp->ghnp', weights, lower_states, precision=best_precision)
        upper_excl = exclusive.reshape(groups, 2, half, heads)[:, 1]
        carry = jnp.exp(upper_excl - lower_end[:, None, :])
        c_upper = c_blocks.reshape(groups, 2, half, length, state_size)[:, 1]
        reads = jnp.einsum('gitn,ghnp->githp', c_upper, summed, precision=best_precision)
        cum_upper = cum.reshape(groups, 2, half, length, heads)[:, 1]
        lam_upper = lam_blocks.reshape(groups, 2, half, length, heads, LEVELS)[:, 1, :, :, :, level]
        scale = carry[:, :, None, :] * jnp.exp(cum_upper) * lam_upper
        shaped = y_all.reshape(groups, 2, half, length, heads, head_size)
        y_all = shaped.at[:, 1].add(reads * scale[..., None]).reshape(blocks, length, heads, head_size)
    y_flat = y_all.reshape(seqlen, inner)
    gated = y_flat * jax.nn.silu(z_gate)
    normed = (gated * lax.rsqrt(lax.optimization_barrier(jnp.mean(gated * gated, axis=1, keepdims=True)) + EPS) * gain_gate).astype(jnp.bfloat16)
    return (hidden + jnp.dot(normed, w_out, preferred_element_type=jnp.float32)).astype(jnp.bfloat16)

def reference(acts, in_proj, out_proj, conv_weight, conv_bias, dt_bias, decay_rate, skip_gain, level_bias, norm_gain, gate_gain):
    results = []
    for section_id in range(SECTIONS):
        results.append(mixer(acts[section_id], in_proj[section_id], out_proj[section_id], conv_weight[section_id], conv_bias[section_id], dt_bias[section_id], decay_rate[section_id], skip_gain[section_id], level_bias[section_id], norm_gain[section_id], gate_gain[section_id]))
    stacked = jnp.stack(results, axis=0)
    return jnp.roll(stacked, 1, axis=0)
```

```python
import jax
import jax.numpy as jnp
from jax import lax
from jax.experimental import pallas as pl
from jax.experimental.pallas import tpu as pltpu
from jax.sharding import PartitionSpec as P

EPS = 1e-05
F32 = jnp.float32
BF = jnp.bfloat16


NX, NZ, NY = 4, 8, 4
ROWS = 256
HEADS = 8
HD = 64
XW = HEADS * HD
NS = 128
HALO = 16
TOK = NY * ROWS
WA, WB = 768, 640
EXT = ROWS + HALO
SPLIT = 144
KX = 512


def route(move):
    pairs = []
    for x in range(NX):
        for z in range(NZ):
            for y in range(NY):
                a, b, c = move(x, z, y)
                pairs.append(
                    ((x * NZ + z) * NY + y, ((a % NX) * NZ + b % NZ) * NY + c % NY)
                )
    return pairs


X_UP = route(lambda x, z, y: (x + 1, z, y))
X_DOWN = route(lambda x, z, y: (x - 1, z, y))
Z_UP = route(lambda x, z, y: (x, z + 1, y))
Z_DOWN = route(lambda x, z, y: (x, z - 1, y))
Y_UP = route(lambda x, z, y: (x, z, y + 1))
Y_DOWN = route(lambda x, z, y: (x, z, y - 1))
Y_TWO = route(lambda x, z, y: (x, z, y + 2))
HALO_NEXT = [(i, i + 1) for i in range(NX * NZ * NY - 1)]
EXCHANGES = [
    route(lambda x, z, y: (x, z ^ 1, y)),
    route(lambda x, z, y: (x, z ^ 2, y)),
    route(lambda x, z, y: (x, 7 - z, y)),
    route(lambda x, z, y: (x ^ 1, z, y)),
    route(lambda x, z, y: (3 - x, z, y)),
]


def sent(value, pairs):
    return lax.ppermute(value, "seq", pairs)


def spread(first, stride):
    row = lax.broadcasted_iota(jnp.int32, (128, XW), 0)
    col = lax.broadcasted_iota(jnp.int32, (128, XW), 1)
    return jnp.where(row == first + stride * (col // HD), 1.0, 0.0).astype(BF)


def mm(a, b):
    return jnp.dot(a.astype(BF), b.astype(BF), preferred_element_type=F32)


def softplus(v):
    return jnp.maximum(v, 0.0) + jnp.log1p(jnp.exp(-jnp.abs(v)))


def silu(v):
    half = 0.5 * v
    return half + half * jnp.tanh(half)


def conv_block(wide, taps, bias):
    mixed = bias[0:1, :] + taps[0:1, :] * wide[HALO - 3 : HALO - 3 + ROWS, :]
    for k in range(1, 4):
        mixed = mixed + taps[k : k + 1, :] * wide[HALO - 3 + k : HALO - 3 + k + ROWS, :]
    return silu(mixed)


def part_kernel(rows_ref, own_ref, below_ref, above_ref, out_ref):
    total = None
    for k, w_ref in enumerate((own_ref, below_ref, above_ref)):
        there = rows_ref[0, :, k * KX : (k + 1) * KX]
        part = jnp.dot(there, w_ref[...], preferred_element_type=F32)
        total = part if total is None else total + part
    out_ref[0] = total


def run_part(rows, own, below, above, name):
    width = own.shape[1]
    return pl.pallas_call(
        part_kernel,
        grid=(NY,),
        in_specs=[
            pl.BlockSpec((1, EXT, 3 * KX), lambda j: (j, 0, 0)),
            whole(KX, width), whole(KX, width), whole(KX, width),
        ],
        out_specs=pl.BlockSpec((1, EXT, width), lambda j: (j, 0, 0)),
        out_shape=jax.ShapeDtypeStruct((NY, EXT, width), F32),
        name=name,
    )(rows, own, below, above)


def finished(part_ref, rows_ref, fa_ref, fb_ref):
    far = rows_ref[0]
    total = (
        part_ref[0]
        + jnp.dot(far[:, : KX // 2], fa_ref[...], preferred_element_type=F32)
        + jnp.dot(far[:, KX // 2 :], fb_ref[...], preferred_element_type=F32)
    )
    return total.astype(BF).astype(F32)


def finished_specs(width):
    return [
        pl.BlockSpec((1, EXT, width), lambda j: (j, 0, 0)),
        pl.BlockSpec((1, EXT, KX), lambda j: (j, 0, 3)),
        whole(KX // 2, width), whole(KX // 2, width),
    ]


def whole(*shape):
    return pl.BlockSpec(shape, lambda j: (0,) * len(shape))


def rows_of(width):
    return pl.BlockSpec((ROWS, width), lambda j: (j, 0))


def shape_of(dtype, *shape):
    return jax.ShapeDtypeStruct(shape, dtype)


def state_kernel(
    part_ref, rows_ref, fa_ref, fb_ref, taps_ref, bias_ref, small_bias_ref, rate_ref, spread_ref,
    xs_ref, b_ref, sp_ref, cum_ref, e2_ref, sc_ref, row_ref, s_ref, pair_ref, state_ref, logs_ref, msg_ref,
    wide_ref, acc_ref, carry_ref,
):
    j = pl.program_id(0)

    @pl.when(j == 0)
    def _():
        acc_ref[...] = jnp.zeros_like(acc_ref)
        carry_ref[...] = jnp.zeros_like(carry_ref)
        logs_ref[...] = jnp.zeros_like(logs_ref)

    p = finished(part_ref, rows_ref, fa_ref, fb_ref)
    wide_ref[...] = p[:, : XW + NS]
    mixed = conv_block(wide_ref, taps_ref, bias_ref)
    xs = mixed[:, :XW]
    b_mat = mixed[:, XW:]
    sp = softplus(p[HALO:, XW + NS :] + small_bias_ref[0:1, :])
    g = -sp * rate_ref[0:1, :]
    row = lax.broadcasted_iota(jnp.int32, (ROWS, ROWS), 0)
    col = lax.broadcasted_iota(jnp.int32, (ROWS, ROWS), 1)
    tri = jnp.where(col <= row, 1.0, 0.0).astype(BF)
    g0 = g.astype(BF)
    r1 = g - g0.astype(F32)
    g1 = r1.astype(BF)
    g2 = r1 - g1.astype(F32)
    cum = mm(tri, g0) + mm(tri, g1) + mm(tri, g2)
    last = cum[ROWS - 1 : ROWS, :]
    tail = jnp.exp(last - cum) * sp
    head_spread = spread_ref[8]
    xt = xs * mm(tail, head_spread)
    state = mm(b_mat.T, xt)
    last8 = jnp.broadcast_to(last, (16, 128))
    hi = last8.astype(BF)
    rest = last8 - hi.astype(F32)
    mid = rest.astype(BF)
    low = rest - mid.astype(F32)
    last_wide = mm(hi, head_spread) + mm(mid, head_spread) + mm(low, head_spread)
    acc = jnp.exp(last_wide[0:1, :]) * acc_ref[...] + state
    acc_ref[...] = acc
    group = carry_ref[0:1, :]
    pair = jnp.where(j == 2, 0.0, carry_ref[1:2, :])
    e2_ref[...] = jnp.exp(cum + pair)
    lane = lax.broadcasted_iota(jnp.int32, (128, 128), 1)
    src = lax.broadcasted_iota(jnp.int32, (128, 128), 0)
    to_levels = jnp.where(src - HEADS * 8 == lane // 8, 1.0, 0.0)
    sc_ref[...] = (sp * mm(jnp.exp(cum + group), to_levels)).astype(BF)
    carry_ref[0:1, :] = group + last
    carry_ref[1:2, :] = pair + last
    xs_ref[...] = xs
    b_ref[...] = b_mat.astype(BF)
    sp_ref[...] = sp
    cum_ref[...] = cum
    row_ref[0] = cum.T[HEADS * 8 : HEADS * 9, :]
    s_ref[0] = state.astype(BF)
    logs_ref[0:1, :] = logs_ref[0:1, :] + last_wide[0:1, :]

    @pl.when(j == 1)
    def _():
        pair_ref[...] = acc.astype(BF)

    @pl.when(j == NY - 1)
    def _():
        state_ref[...] = acc
        pack_message(msg_ref, acc, logs_ref[0:1, :])


def pack_message(msg_ref, state, log):
    msg_ref[0:NS, :] = state.astype(BF)
    hi = log.astype(BF).astype(F32)
    row = lax.broadcasted_iota(jnp.int32, (16, XW), 0)
    both = jnp.where(row == 0, hi, jnp.where(row == 1, log - hi, 0.0))
    msg_ref[NS:, :] = both.astype(BF)


def run_state(part, rows, far_a, far_b, taps, bias, small_bias, rate, spreads):
    return pl.pallas_call(
        state_kernel,
        grid=(NY,),
        in_specs=[
            *finished_specs(WA),
            whole(4, XW + NS), whole(1, XW + NS), whole(1, 128), whole(1, 128), whole(9, 128, XW),
        ],
        out_specs=[
            rows_of(XW), rows_of(NS), rows_of(128), rows_of(128), rows_of(128), rows_of(128),
            pl.BlockSpec((1, HEADS, ROWS), lambda j: (j, 0, 0)),
            pl.BlockSpec((1, NS, XW), lambda j: (j, 0, 0)),
            whole(NS, XW), whole(NS, XW), whole(8, XW), whole(NS + 16, XW),
        ],
        out_shape=[
            shape_of(F32, TOK, XW), shape_of(BF, TOK, NS), shape_of(F32, TOK, 128),
            shape_of(F32, TOK, 128), shape_of(F32, TOK, 128), shape_of(BF, TOK, 128),
            shape_of(F32, NY, HEADS, ROWS), shape_of(BF, NY, NS, XW),
            shape_of(BF, NS, XW), shape_of(F32, NS, XW), shape_of(F32, 8, XW), shape_of(BF, NS + 16, XW),
        ],
        scratch_shapes=[
            pltpu.VMEM((ROWS + HALO, XW + NS), F32),
            pltpu.VMEM((NS, XW), F32),
            pltpu.VMEM((8, 128), F32),
        ],
        name="conv_states",
    )(part, rows, far_a, far_b, taps, bias, small_bias, rate, spreads)


def intra_kernel(
    part_ref, rows_ref, fa_ref, fb_ref, taps_ref, bias_ref, skip_ref,
    xs_ref, b_ref, sp_ref, cum_ref, e2_ref, row_ref, s1_ref, s2_ref, spread_ref,
    y_ref, c_ref, z_ref, wide_ref,
):
    j = pl.program_id(0)
    p = finished(part_ref, rows_ref, fa_ref, fb_ref)
    z_ref[...] = p[HALO:, :XW].astype(BF)
    wide_ref[...] = p[:, XW:]
    c_mat = conv_block(wide_ref, taps_ref, bias_ref).astype(BF)
    c_ref[...] = c_mat
    xs = xs_ref[...]
    sp = sp_ref[...].astype(BF)
    cum = cum_ref[...]
    scores = lax.dot_general(
        c_mat, b_ref[...], (((1,), (1,)), ((), ())), preferred_element_type=F32
    )
    row = lax.broadcasted_iota(jnp.int32, (ROWS, ROWS), 0)
    col = lax.broadcasted_iota(jnp.int32, (ROWS, ROWS), 1)
    causal = col <= row
    head_spread = spread_ref[8]
    xd = (xs * mm(sp, head_spread)).astype(BF)
    parts = []
    for h in range(HEADS):
        lane = HEADS * 8 + h
        diff = cum[:, lane : lane + 1] - row_ref[0, h : h + 1, :]
        decay = jnp.exp(jnp.where(causal, diff, -1e30)) * scores
        parts.append(mm(decay, xd[:, h * HD : (h + 1) * HD]))
    y = jnp.concatenate(parts, axis=1) * mm(sp, spread_ref[0])
    y = y + skip_ref[0:1, :] * xs
    odd = (j % 2).astype(F32)
    late = (j // 2).astype(F32)
    one = mm(sp, spread_ref[1]) * mm(jnp.exp(cum), head_spread)
    y = y + mm(c_mat, s1_ref[0]) * (one * odd)
    two = mm(sp, spread_ref[2]) * mm(e2_ref[...], head_spread)
    y = y + mm(c_mat, s2_ref[...]) * (two * late)
    y_ref[...] = y


def run_intra(part, rows, far_a, far_b, taps, bias, skip, xs, b_mat, sp, cum, e2, row, states, pair, spreads):
    return pl.pallas_call(
        intra_kernel,
        grid=(NY,),
        in_specs=[
            *finished_specs(WB),
            whole(4, NS), whole(1, NS), whole(1, XW),
            rows_of(XW), rows_of(NS), rows_of(128), rows_of(128), rows_of(128),
            pl.BlockSpec((1, HEADS, ROWS), lambda j: (j, 0, 0)),
            pl.BlockSpec((1, NS, XW), lambda j: ((j // 2) * 2, 0, 0)),
            whole(NS, XW), whole(9, 128, XW),
        ],
        out_specs=[rows_of(XW), rows_of(NS), rows_of(XW)],
        out_shape=[shape_of(F32, TOK, XW), shape_of(BF, TOK, NS), shape_of(BF, TOK, XW)],
        scratch_shapes=[pltpu.VMEM((ROWS + HALO, NS), F32)],
        name="intra_block",
    )(part, rows, far_a, far_b, taps, bias, skip, xs, b_mat, sp, cum, e2, row, states, pair, spreads)


def merge_kernel(bit_ref, got_ref, state_ref, logs_ref, msg_ref, new_ref, new_logs_ref, bucket_ref):
    upper = bit_ref[0] == 1
    other = got_ref[0:NS, :].astype(F32)
    tail = got_ref[NS:, :].astype(F32)
    other_log = tail[0:1, :] + tail[1:2, :]
    log = logs_ref[0:1, :]
    before = logs_ref[1:2, :]
    bucket = jnp.where(upper, jnp.exp(before), 0.0) * other
    bucket_ref[...] = bucket.astype(BF)
    state = (
        jnp.where(upper, jnp.exp(log), 1.0) * other
        + jnp.where(upper, 1.0, jnp.exp(other_log)) * state_ref[...]
    )
    new_ref[...] = state
    log = log + other_log
    new_logs_ref[...] = jnp.zeros_like(new_logs_ref)
    new_logs_ref[0:1, :] = log
    new_logs_ref[1:2, :] = jnp.where(upper, before + other_log, before)
    pack_message(msg_ref, state, log)


def run_merge(bit, got, state, logs):
    vmem = pl.BlockSpec(memory_space=pltpu.VMEM)
    return pl.pallas_call(
        merge_kernel,
        in_specs=[pl.BlockSpec(memory_space=pltpu.SMEM), vmem, vmem, vmem],
        out_specs=[vmem] * 4,
        out_shape=[
            shape_of(BF, NS + 16, XW), shape_of(F32, NS, XW), shape_of(F32, 8, XW), shape_of(BF, NS, XW),
        ],
        name="merge",
    )(bit.reshape(1), got, state, logs)


def cross_kernel(y_ref, c_ref, sc_ref, z_ref, k3, k4, k5, k6, k7, spread_ref, q_ref):
    c_mat = c_ref[...]
    scale = sc_ref[...]
    y = y_ref[...]
    for level, bucket in ((3, k3), (4, k4), (5, k5), (6, k6), (7, k7)):
        y = y + mm(c_mat, bucket[...]) * mm(scale, spread_ref[level])
    q_ref[...] = (y * silu(z_ref[...].astype(F32))).astype(BF)


def run_cross(y, c_mat, sc, z, buckets, spreads):
    return pl.pallas_call(
        cross_kernel,
        grid=(NY,),
        in_specs=[rows_of(XW), rows_of(NS), rows_of(128), rows_of(XW)]
        + [whole(NS, XW)] * 5
        + [whole(9, 128, XW)],
        out_specs=rows_of(XW),
        out_shape=shape_of(BF, TOK, XW),
        name="cross_gate",
    )(y, c_mat, sc, z, *buckets, spreads)


def out_kernel(at_ref, q0, q1, q2, q3, gain_ref, w_ref, acts_ref, out_ref, acc_ref, scale_ref):
    k = pl.program_id(0)
    blocks = (q0, q1, q2, q3)

    @pl.when(k == 0)
    def _():
        parts = [q[...].astype(F32) for q in blocks]
        square = sum(jnp.sum(v * v, axis=1, keepdims=True) for v in parts)
        scale = lax.rsqrt(square / (NY * XW) + EPS)
        scale_ref[...] = jnp.broadcast_to(scale, scale_ref.shape)
        acc_ref[...] = acts_ref[...].astype(F32)

    for i, q in enumerate(blocks):

        @pl.when(k == i)
        def _(q=q):
            n = q[...].astype(F32) * scale_ref[:, 0:1] * gain_ref[0:1, :]
            acc_ref[...] += jnp.dot(n.astype(BF), w_ref[...], preferred_element_type=F32)

    @pl.when(k == NY - 1)
    def _():
        out_ref[...] = acc_ref[...].astype(BF)


def run_out(at, blocks, gain, weight, acts):
    width = weight.shape[1]
    fixed = lambda *shape: pl.BlockSpec(shape, lambda k, at: (0,) * len(shape))
    return pl.pallas_call(
        out_kernel,
        grid_spec=pltpu.PrefetchScalarGridSpec(
            num_scalar_prefetch=1,
            grid=(NY,),
            in_specs=[fixed(ROWS, XW)] * 4
            + [
                pl.BlockSpec((1, XW), lambda k, at: (0, at[k])),
                pl.BlockSpec((XW, width), lambda k, at: (at[k], 0)),
                fixed(ROWS, width),
            ],
            out_specs=fixed(ROWS, width),
            scratch_shapes=[pltpu.VMEM((ROWS, width), F32), pltpu.VMEM((ROWS, 128), F32)],
        ),
        out_shape=shape_of(BF, ROWS, width),
        name="gate_out",
    )(at, *blocks, gain, weight, acts)


def norm_kernel(at_ref, halo_ref, acts_ref, gain_ref, out_ref, full_ref):
    for start, ref in ((0, halo_ref), (HALO, acts_ref)):
        v = ref[...].astype(F32)
        scale = lax.rsqrt(jnp.mean(v * v, axis=1, keepdims=True) + EPS)
        full_ref[start : start + v.shape[0], :] = v * scale * gain_ref[0:1, :]
    for k in range(NX):
        start = pl.multiple_of(at_ref[k] * KX, KX)
        part = pltpu.roll(full_ref[:, pl.ds(start, KX)], at_ref[NX], 1)
        out_ref[:, k * KX : (k + 1) * KX] = part.astype(BF)


def run_norm(at, halo, acts, gain):
    vmem = pl.BlockSpec(memory_space=pltpu.VMEM)
    return pl.pallas_call(
        norm_kernel,
        in_specs=[pl.BlockSpec(memory_space=pltpu.SMEM), vmem, vmem, vmem],
        out_specs=vmem,
        out_shape=shape_of(BF, EXT, acts.shape[1]),
        scratch_shapes=[pltpu.VMEM((EXT, acts.shape[1]), F32)],
        name="norm_rows",
    )(at, halo, acts, gain)


def columns_kernel(y_ref, shard_ref, o0, o1, o2, o3, all_ref):
    shard = shard_ref[...]
    for t in range(NY):
        x0, z0 = t * XW, 2304 + t * XW
        dt0, lv0 = 4352 + t * HEADS, 4384 + t * HEADS * 8
        all_ref[t, :, 0:XW] = shard[:, x0 : x0 + XW]
        all_ref[t, :, XW : XW + NS] = shard[:, 2048 : 2048 + NS]
        all_ref[t, :, XW + NS : WA] = jnp.concatenate(
            [
                shard[:, lv0 : lv0 + HEADS * 8].astype(F32),
                shard[:, dt0 : dt0 + HEADS].astype(F32),
                jnp.zeros((shard.shape[0], 128 - HEADS * 9), F32),
            ],
            axis=1,
        ).astype(BF)
        all_ref[t, :, WA : WA + XW] = shard[:, z0 : z0 + XW]
        all_ref[t, :, WA + XW :] = shard[:, 2048 + NS : 2304]
    for k, out in enumerate((o0, o1, o2, o3)):
        out[...] = all_ref[(y_ref[0] + k) % NY]


def run_columns(y, shard):
    vmem = pl.BlockSpec(memory_space=pltpu.VMEM)
    rows = shard.shape[0]
    return pl.pallas_call(
        columns_kernel,
        in_specs=[pl.BlockSpec(memory_space=pltpu.SMEM), vmem],
        out_specs=[vmem] * 4,
        out_shape=[shape_of(BF, rows, WA + WB)] * 4,
        scratch_shapes=[pltpu.VMEM((NY, rows, WA + WB), BF)],
        name="split_columns",
    )(y.reshape(1), shard)


def join_kernel(y_ref, b0, b1, b2, b3, out_ref):
    rows = b0.shape[0]
    for back, block in ((0, b0), (3, b1), (2, b2), (1, b3)):
        start = pl.multiple_of(((y_ref[0] + back) % NY) * rows, rows)
        out_ref[pl.ds(start, rows), :] = block[...]


def run_join(y, blocks):
    vmem = pl.BlockSpec(memory_space=pltpu.VMEM)
    rows, width = blocks[0].shape
    return pl.pallas_call(
        join_kernel,
        in_specs=[pl.BlockSpec(memory_space=pltpu.SMEM)] + [vmem] * 4,
        out_specs=vmem,
        out_shape=shape_of(BF, NY * rows, width),
        name="join_columns",
    )(y.reshape(1), *blocks)


def together(*values):
    return lax.optimization_barrier(values)


def ring_z(block):
    up, down = [block], [block]
    for k in range(4):
        up.append(sent(up[-1], Z_UP))
        if k < 3:
            down.append(sent(down[-1], Z_DOWN))
    return down + [up[4], up[3], up[2], up[1]]


def ring_four(block, up, down):
    below = sent(block, up)
    above = sent(block, down)
    half = block.shape[0] // 2
    return below, above, lambda: (sent(below[:half], up), sent(above[half:], down))


def per_device(
    acts,
    in_proj,
    out_proj,
    conv_weight,
    conv_bias,
    dt_bias,
    decay_rate,
    skip_gain,
    level_bias,
    norm_gain,
    gate_gain,
):
    index = lax.axis_index("seq")
    y = index % NY
    z = (index // NY) % NZ
    x = index // (NY * NZ)
    halo = sent(acts[0, ROWS - HALO :], HALO_NEXT)
    w0, w1, w2, w3 = run_columns(y, in_proj[0])
    columns = run_join(y, (w0, sent(w1, Y_UP), sent(w2, Y_TWO), sent(w3, Y_DOWN)))
    order = jnp.stack([x, (x + 3) % NX, (x + 1) % NX, (x + 2) % NX, (512 - 64 * z) % 512])
    u = run_norm(order, halo, acts[0], norm_gain)

    piece = lambda v, width: lax.dynamic_slice_in_dim(v, y * width, width, v.ndim - 1)
    taps_a = jnp.concatenate(
        [piece(conv_weight[0, :, :2048], XW), conv_weight[0, :, 2048 : 2048 + NS]], axis=1
    )
    bias_a = jnp.concatenate(
        [piece(conv_bias[:, :2048], XW), conv_bias[:, 2048 : 2048 + NS]], axis=1
    )
    pad = jnp.zeros((1, 128 - HEADS * 9), F32)
    small_bias = jnp.concatenate(
        [piece(level_bias, HEADS * 8), piece(dt_bias, HEADS), pad], axis=1
    )
    rate = jnp.concatenate(
        [jnp.zeros((1, HEADS * 8), F32), piece(decay_rate, HEADS), pad], axis=1
    )
    skip = jnp.repeat(piece(skip_gain, HEADS), HD, axis=1)
    (zero,) = together(jnp.zeros((), jnp.int32))
    spreads = jnp.stack([spread(zero + k, 8) for k in range(8)] + [spread(zero + HEADS * 8, 1)])

    columns, u = together(columns, u)
    blocks = ring_z(columns)
    below, above, _ = ring_four(u, Y_UP, Y_DOWN)
    below, above, blocks[3] = together(below, above, blocks[3])
    far_lo, far_hi = sent(below[:SPLIT], Y_UP), sent(above[SPLIT:], Y_DOWN)
    by_a = jnp.concatenate([block[:, :WA] for block in blocks], axis=0)
    by_b = jnp.concatenate([block[:, WA:] for block in blocks], axis=0)

    with jax.named_scope("near_first"):
        a_below, a_above, a_far = ring_four(by_a, X_UP, X_DOWN)
    rows = jnp.zeros((NY, EXT, u.shape[1]), BF)
    place = lambda v, k, r: lax.dynamic_update_slice(rows, v[None], ((y + k) % NY, zero + r, zero))
    rows = place(u, 0, 0)
    rows = place(below, 3, 0)
    rows = place(above, 1, 0)
    rows = place(far_lo, 2, 0)
    rows = place(far_hi, 2, SPLIT)
    with jax.named_scope("far_first"):
        fa_a, fb_a = a_far()
    with jax.named_scope("do_first"):
        part_a = run_part(rows, by_a, a_below, a_above, "project_first")

    by_b, fa_a, fb_a = together(by_b, fa_a, fb_a)
    with jax.named_scope("near_second"):
        b_below, b_above, b_far = ring_four(by_b, X_UP, X_DOWN)
    xs, b_mat, sp, cum, e2, sc, row, states, pair, state, logs, message = run_state(
        part_a, rows, fa_a, fb_a, taps_a, bias_a, small_bias, rate, spreads
    )
    with jax.named_scope("far_second"):
        fa_b, fb_b = b_far()
    with jax.named_scope("do_second"):
        part_b = run_part(rows, by_b, b_below, b_above, "project_second")

    bits = [z & 1, (z >> 1) & 1, (z >> 2) & 1, x & 1, (x >> 1) & 1]
    buckets = []
    for k, (bit, pairs) in enumerate(zip(bits, EXCHANGES, strict=True)):
        with jax.named_scope(f"round_{k}"):
            got = sent(message, pairs)
        message, state, logs, bucket = run_merge(bit, got, state, logs)
        buckets.append(bucket)

    y_part, c_mat, z_cols = run_intra(
        part_b, rows, fa_b, fb_b, conv_weight[0, :, 2048 + NS :], conv_bias[:, 2048 + NS :], skip,
        xs, b_mat, sp, cum, e2, row, states, pair, spreads,
    )
    q = run_cross(y_part, c_mat, sc, z_cols, buckets, spreads)
    take = lambda k: lax.dynamic_slice_in_dim(q, ((y + k) % NY) * ROWS, ROWS, 0)
    far = sent(take(2), Y_TWO)
    blocks = (take(0), sent(take(1), Y_UP), far, sent(take(3), Y_DOWN))
    heads_at = jnp.stack([y, (y + 3) % NY, (y + 2) % NY, (y + 1) % NY])
    result = run_out(heads_at, blocks, gate_gain, out_proj[0], acts[0])
    return lax.ppermute(result, "section", [(0, 1), (1, 0)])[None]


def solution(mesh):
    return jax.shard_map(
        per_device,
        mesh=mesh,
        in_specs=(
            P("section", "seq", None),
            P("section", "seq", None),
            P("section", None, None),
            P("section", None, None),
            P("section", None),
            P("section", None),
            P("section", None),
            P("section", None),
            P("section", None),
            P("section", None),
            P("section", None),
        ),
        out_specs=P("section", "seq", None),
        check_vma=False,
    )
```

```python
import jax
import jax.numpy as jnp
from jax import lax
from jax.experimental import pallas as pl
from jax.experimental.pallas import tpu as pltpu
from jax.sharding import PartitionSpec as P

EPS = 1e-05
F32 = jnp.float32
BF = jnp.bfloat16


NX, NZ, NY = 4, 8, 4
ROWS = 256
HEADS = 8
HD = 64
XW = HEADS * HD
NS = 128
HALO = 16
WA, WB = 768, 640
EXT = ROWS + HALO
SPLIT = 144
KX = 512


def route(move):
    pairs = []
    for x in range(NX):
        for z in range(NZ):
            for y in range(NY):
                a, b, c = move(x, z, y)
                pairs.append(
                    ((x * NZ + z) * NY + y, ((a % NX) * NZ + b % NZ) * NY + c % NY)
                )
    return pairs


X_UP = route(lambda x, z, y: (x + 1, z, y))
X_DOWN = route(lambda x, z, y: (x - 1, z, y))
Z_UP = route(lambda x, z, y: (x, z + 1, y))
Z_DOWN = route(lambda x, z, y: (x, z - 1, y))
Y_UP = route(lambda x, z, y: (x, z, y + 1))
Y_DOWN = route(lambda x, z, y: (x, z, y - 1))
Y_TWO = route(lambda x, z, y: (x, z, y + 2))
HALO_NEXT = [(i, i + 1) for i in range(NX * NZ * NY - 1)]
EXCHANGES = [
    route(lambda x, z, y: (x, z ^ 1, y)),
    route(lambda x, z, y: (x, z ^ 2, y)),
    route(lambda x, z, y: (x, 7 - z, y)),
    route(lambda x, z, y: (x ^ 1, z, y)),
    route(lambda x, z, y: (3 - x, z, y)),
]


def sent(value, pairs):
    return lax.ppermute(value, "seq", pairs)


def spread(first, stride):
    row = lax.broadcasted_iota(jnp.int32, (128, XW), 0)
    col = lax.broadcasted_iota(jnp.int32, (128, XW), 1)
    return jnp.where(row == first + stride * (col // HD), 1.0, 0.0).astype(BF)


def mm(a, b):
    return jnp.dot(a.astype(BF), b.astype(BF), preferred_element_type=F32)


def softplus(v):
    return jnp.maximum(v, 0.0) + jnp.log1p(jnp.exp(-jnp.abs(v)))


def silu(v):
    half = 0.5 * v
    return half + half * jnp.tanh(half)


def conv_block(wide, taps, bias):
    mixed = bias[0:1, :] + taps[0:1, :] * wide[HALO - 3 : HALO - 3 + ROWS, :]
    for k in range(1, 4):
        mixed = mixed + taps[k : k + 1, :] * wide[HALO - 3 + k : HALO - 3 + k + ROWS, :]
    return silu(mixed)


def shape_of(dtype, *shape):
    return pltpu.VMEM(shape, dtype)


def near(value):
    return pltpu.with_memory_space_constraint(value, pltpu.VMEM)


def run(kernel, scalars, arrays, outs, scratch=()):
    smem = pl.BlockSpec(memory_space=pltpu.SMEM)
    vmem = pl.BlockSpec(memory_space=pltpu.VMEM)
    return pl.pallas_call(
        kernel,
        in_specs=[smem] * len(scalars) + [vmem] * len(arrays),
        out_specs=[vmem] * len(outs),
        out_shape=outs,
        scratch_shapes=list(scratch),
        compiler_params=pltpu.CompilerParams(vmem_limit_bytes=10 << 20),
    )(*scalars, *map(near, arrays))


def each_block(body):
    def step(j, carry):
        body(j)
        return carry

    lax.fori_loop(0, NY, step, 0)


def part_kernel(rows_ref, own_ref, below_ref, above_ref, out_ref):
    def block(j):
        total = None
        for k, w_ref in enumerate((own_ref, below_ref, above_ref)):
            there = rows_ref[j, :, k * KX : (k + 1) * KX]
            part = jnp.dot(there, w_ref[...], preferred_element_type=F32)
            total = part if total is None else total + part
        out_ref[j] = total

    each_block(block)


def run_part(rows, own, below, above):
    width = own.shape[1]
    return run(part_kernel, (), (rows, own, below, above), [shape_of(F32, NY, EXT, width)])[0]


def stack_kernel(y_ref, own_ref, below_ref, above_ref, lo_ref, hi_ref, out_ref):
    y = y_ref[0]
    out_ref[y] = own_ref[...]
    out_ref[(y + 3) % NY] = below_ref[...]
    out_ref[(y + 1) % NY] = above_ref[...]
    out_ref[(y + 2) % NY, 0:SPLIT, :] = lo_ref[...]
    out_ref[(y + 2) % NY, SPLIT:, :] = hi_ref[...]


def finished(part_ref, rows_ref, fa_ref, fb_ref, j):
    total = (
        part_ref[j]
        + jnp.dot(rows_ref[j, :, 3 * KX : 3 * KX + KX // 2], fa_ref[...], preferred_element_type=F32)
        + jnp.dot(rows_ref[j, :, 3 * KX + KX // 2 :], fb_ref[...], preferred_element_type=F32)
    )
    return total.astype(BF).astype(F32)


def state_kernel(
    part_ref, rows_ref, fa_ref, fb_ref, taps_ref, bias_ref, small_bias_ref, rate_ref, spread_ref,
    xs_ref, b_ref, sp_ref, cum_ref, e2_ref, sc_ref, row_ref, s_ref, pair_ref, state_ref, logs_ref, msg_ref,
    wide_ref, acc_ref, carry_ref,
):
    acc_ref[...] = jnp.zeros_like(acc_ref)
    carry_ref[...] = jnp.zeros_like(carry_ref)
    logs_ref[...] = jnp.zeros_like(logs_ref)

    def block(j):
        p = finished(part_ref, rows_ref, fa_ref, fb_ref, j)
        wide_ref[...] = p[:, : XW + NS]
        mixed = conv_block(wide_ref, taps_ref, bias_ref)
        xs = mixed[:, :XW]
        b_mat = mixed[:, XW:]
        sp = softplus(p[HALO:, XW + NS :] + small_bias_ref[0:1, :])
        g = -sp * rate_ref[0:1, :]
        row = lax.broadcasted_iota(jnp.int32, (ROWS, ROWS), 0)
        col = lax.broadcasted_iota(jnp.int32, (ROWS, ROWS), 1)
        tri = jnp.where(col <= row, 1.0, 0.0).astype(BF)
        g0 = g.astype(BF)
        r1 = g - g0.astype(F32)
        g1 = r1.astype(BF)
        g2 = r1 - g1.astype(F32)
        cum = mm(tri, g0) + mm(tri, g1) + mm(tri, g2)
        last = cum[ROWS - 1 : ROWS, :]
        tail = jnp.exp(last - cum) * sp
        head_spread = spread_ref[8]
        xt = xs * mm(tail, head_spread)
        state = mm(b_mat.T, xt)
        last8 = jnp.broadcast_to(last, (16, 128))
        hi = last8.astype(BF)
        rest = last8 - hi.astype(F32)
        mid = rest.astype(BF)
        low = rest - mid.astype(F32)
        last_wide = mm(hi, head_spread) + mm(mid, head_spread) + mm(low, head_spread)
        acc = jnp.exp(last_wide[0:1, :]) * acc_ref[...] + state
        acc_ref[...] = acc
        group = carry_ref[0:1, :]
        pair = jnp.where(j == 2, 0.0, carry_ref[1:2, :])
        e2_ref[j] = jnp.exp(cum + pair)
        lane = lax.broadcasted_iota(jnp.int32, (128, 128), 1)
        src = lax.broadcasted_iota(jnp.int32, (128, 128), 0)
        to_levels = jnp.where(src - HEADS * 8 == lane // 8, 1.0, 0.0)
        sc_ref[j] = (sp * mm(jnp.exp(cum + group), to_levels)).astype(BF)
        carry_ref[0:1, :] = group + last
        carry_ref[1:2, :] = pair + last
        xs_ref[j] = xs
        b_ref[j] = b_mat.astype(BF)
        sp_ref[j] = sp
        cum_ref[j] = cum
        row_ref[j] = cum.T[HEADS * 8 : HEADS * 9, :]
        s_ref[j] = state.astype(BF)
        logs_ref[0:1, :] = logs_ref[0:1, :] + last_wide[0:1, :]

        @pl.when(j == 1)
        def _():
            pair_ref[...] = acc.astype(BF)

        @pl.when(j == NY - 1)
        def _():
            state_ref[...] = acc
            pack_message(msg_ref, acc, logs_ref[0:1, :])

    each_block(block)


def pack_message(msg_ref, state, log):
    msg_ref[0:NS, :] = state.astype(BF)
    hi = log.astype(BF).astype(F32)
    row = lax.broadcasted_iota(jnp.int32, (16, XW), 0)
    both = jnp.where(row == 0, hi, jnp.where(row == 1, log - hi, 0.0))
    msg_ref[NS:, :] = both.astype(BF)


def run_state(part, rows, far_a, far_b, taps, bias, small_bias, rate, spreads):
    return run(
        state_kernel,
        (),
        (part, rows, far_a, far_b, taps, bias, small_bias, rate, spreads),
        [
            shape_of(F32, NY, ROWS, XW), shape_of(BF, NY, ROWS, NS), shape_of(F32, NY, ROWS, 128),
            shape_of(F32, NY, ROWS, 128), shape_of(F32, NY, ROWS, 128), shape_of(BF, NY, ROWS, 128),
            shape_of(F32, NY, HEADS, ROWS), shape_of(BF, NY, NS, XW),
            shape_of(BF, NS, XW), shape_of(F32, NS, XW), shape_of(F32, 8, XW), shape_of(BF, NS + 16, XW),
        ],
        [
            pltpu.VMEM((EXT, XW + NS), F32),
            pltpu.VMEM((NS, XW), F32),
            pltpu.VMEM((8, 128), F32),
        ],
    )


def intra_kernel(
    part_ref, rows_ref, fa_ref, fb_ref, taps_ref, bias_ref, skip_ref,
    xs_ref, b_ref, sp_ref, cum_ref, e2_ref, row_ref, s1_ref, s2_ref, spread_ref,
    y_ref, c_ref, z_ref, wide_ref,
):
    def block(j):
        p = finished(part_ref, rows_ref, fa_ref, fb_ref, j)
        z_ref[j] = p[HALO:, :XW].astype(BF)
        wide_ref[...] = p[:, XW:]
        c_mat = conv_block(wide_ref, taps_ref, bias_ref).astype(BF)
        c_ref[j] = c_mat
        xs = xs_ref[j]
        sp = sp_ref[j].astype(BF)
        cum = cum_ref[j]
        scores = lax.dot_general(
            c_mat, b_ref[j], (((1,), (1,)), ((), ())), preferred_element_type=F32
        )
        row = lax.broadcasted_iota(jnp.int32, (ROWS, ROWS), 0)
        col = lax.broadcasted_iota(jnp.int32, (ROWS, ROWS), 1)
        causal = col <= row
        head_spread = spread_ref[8]
        xd = (xs * mm(sp, head_spread)).astype(BF)
        parts = []
        for h in range(HEADS):
            lane = HEADS * 8 + h
            diff = cum[:, lane : lane + 1] - row_ref[j, h : h + 1, :]
            decay = jnp.exp(jnp.where(causal, diff, -1e30)) * scores
            parts.append(mm(decay, xd[:, h * HD : (h + 1) * HD]))
        y = jnp.concatenate(parts, axis=1) * mm(sp, spread_ref[0])
        y = y + skip_ref[0:1, :] * xs
        odd = (j % 2).astype(F32)
        late = (j // 2).astype(F32)
        one = mm(sp, spread_ref[1]) * mm(jnp.exp(cum), head_spread)
        y = y + mm(c_mat, s1_ref[(j // 2) * 2]) * (one * odd)
        two = mm(sp, spread_ref[2]) * mm(e2_ref[j], head_spread)
        y = y + mm(c_mat, s2_ref[...]) * (two * late)
        y_ref[j] = y

    each_block(block)


def run_intra(part, rows, far_a, far_b, taps, bias, skip, xs, b_mat, sp, cum, e2, row, states, pair, spreads):
    return run(
        intra_kernel,
        (),
        (part, rows, far_a, far_b, taps, bias, skip, xs, b_mat, sp, cum, e2, row, states, pair, spreads),
        [shape_of(F32, NY, ROWS, XW), shape_of(BF, NY, ROWS, NS), shape_of(BF, NY, ROWS, XW)],
        [pltpu.VMEM((EXT, NS), F32)],
    )


def merge_kernel(bit_ref, got_ref, state_ref, logs_ref, msg_ref, new_ref, new_logs_ref, bucket_ref):
    upper = bit_ref[0] == 1
    other = got_ref[0:NS, :].astype(F32)
    tail = got_ref[NS:, :].astype(F32)
    other_log = tail[0:1, :] + tail[1:2, :]
    log = logs_ref[0:1, :]
    before = logs_ref[1:2, :]
    bucket = jnp.where(upper, jnp.exp(before), 0.0) * other
    bucket_ref[...] = bucket.astype(BF)
    state = (
        jnp.where(upper, jnp.exp(log), 1.0) * other
        + jnp.where(upper, 1.0, jnp.exp(other_log)) * state_ref[...]
    )
    new_ref[...] = state
    log = log + other_log
    new_logs_ref[...] = jnp.zeros_like(new_logs_ref)
    new_logs_ref[0:1, :] = log
    new_logs_ref[1:2, :] = jnp.where(upper, before + other_log, before)
    pack_message(msg_ref, state, log)


def run_merge(bit, got, state, logs):
    return run(
        merge_kernel,
        (bit.reshape(1),),
        (got, state, logs),
        [shape_of(BF, NS + 16, XW), shape_of(F32, NS, XW), shape_of(F32, 8, XW), shape_of(BF, NS, XW)],
    )


def cross_kernel(at_ref, y_ref, c_ref, sc_ref, z_ref, k3, k4, k5, k6, k7, spread_ref, *q_refs):
    for k, q_ref in enumerate(q_refs):
        j = at_ref[k]
        c_mat = c_ref[j]
        scale = sc_ref[j]
        y = y_ref[j]
        for level, bucket in ((3, k3), (4, k4), (5, k5), (6, k6), (7, k7)):
            y = y + mm(c_mat, bucket[...]) * mm(scale, spread_ref[level])
        q_ref[...] = (y * silu(z_ref[j].astype(F32))).astype(BF)


def run_cross(at, y, c_mat, sc, z, buckets, spreads):
    return run(
        cross_kernel,
        (jnp.stack(at),),
        (y, c_mat, sc, z, *buckets, spreads),
        [shape_of(BF, ROWS, XW)] * len(at),
    )


def out_kernel(at_ref, q0, q1, q2, q3, gain_ref, w_ref, acts_ref, out_ref, acc_ref):
    blocks = (q0, q1, q2, q3)
    square = sum(
        jnp.sum(jnp.square(q[...].astype(F32)), axis=1, keepdims=True) for q in blocks
    )
    scale = lax.rsqrt(square / (NY * XW) + EPS)
    acc_ref[...] = acts_ref[...].astype(F32)
    for k, q in enumerate(blocks):
        there = pl.ds(pl.multiple_of(at_ref[k] * XW, XW), XW)
        n = q[...].astype(F32) * scale * gain_ref[0:1, there]
        acc_ref[...] += jnp.dot(n.astype(BF), w_ref[there, :], preferred_element_type=F32)
    out_ref[...] = acc_ref[...].astype(BF)


def run_out(at, blocks, gain, weight, acts):
    width = weight.shape[1]
    return run(
        out_kernel,
        (at,),
        (*blocks, gain, weight, acts),
        [shape_of(BF, ROWS, width)],
        [pltpu.VMEM((ROWS, width), F32)],
    )[0]


def norm_kernel(at_ref, halo_ref, acts_ref, gain_ref, out_ref, full_ref):
    for start, ref in ((0, halo_ref), (HALO, acts_ref)):
        v = ref[...].astype(F32)
        scale = lax.rsqrt(jnp.mean(v * v, axis=1, keepdims=True) + EPS)
        full_ref[start : start + v.shape[0], :] = v * scale * gain_ref[0:1, :]
    for k in range(NX):
        start = pl.multiple_of(at_ref[k] * KX, KX)
        part = pltpu.roll(full_ref[:, pl.ds(start, KX)], at_ref[NX], 1)
        out_ref[:, k * KX : (k + 1) * KX] = part.astype(BF)


def run_norm(at, halo, acts, gain):
    width = acts.shape[1]
    return run(
        norm_kernel,
        (at,),
        (halo, acts, gain),
        [shape_of(BF, EXT, width)],
        [pltpu.VMEM((EXT, width), F32)],
    )[0]


def columns_kernel(y_ref, shard_ref, o0, o1, o2, o3, all_ref):
    shard = shard_ref[...]
    for t in range(NY):
        x0, z0 = t * XW, 2304 + t * XW
        dt0, lv0 = 4352 + t * HEADS, 4384 + t * HEADS * 8
        all_ref[t, :, 0:XW] = shard[:, x0 : x0 + XW]
        all_ref[t, :, XW : XW + NS] = shard[:, 2048 : 2048 + NS]
        all_ref[t, :, XW + NS : WA] = jnp.concatenate(
            [
                shard[:, lv0 : lv0 + HEADS * 8].astype(F32),
                shard[:, dt0 : dt0 + HEADS].astype(F32),
                jnp.zeros((shard.shape[0], 128 - HEADS * 9), F32),
            ],
            axis=1,
        ).astype(BF)
        all_ref[t, :, WA : WA + XW] = shard[:, z0 : z0 + XW]
        all_ref[t, :, WA + XW :] = shard[:, 2048 + NS : 2304]
    for k, out in enumerate((o0, o1, o2, o3)):
        out[...] = all_ref[(y_ref[0] + k) % NY]


def run_columns(y, shard):
    rows = shard.shape[0]
    return run(
        columns_kernel,
        (y.reshape(1),),
        (shard,),
        [shape_of(BF, rows, WA + WB)] * 4,
        [pltpu.VMEM((NY, rows, WA + WB), BF)],
    )


def join_kernel(y_ref, b0, b1, b2, b3, out_ref):
    rows = b0.shape[0]
    for back, block in ((0, b0), (3, b1), (2, b2), (1, b3)):
        start = pl.multiple_of(((y_ref[0] + back) % NY) * rows, rows)
        out_ref[pl.ds(start, rows), :] = block[...]


def run_join(y, blocks):
    rows, width = blocks[0].shape
    return run(join_kernel, (y.reshape(1),), blocks, [shape_of(BF, NY * rows, width)])[0]


def gather_kernel(*refs):
    *blocks, a_ref, b_ref = refs
    rows = blocks[0].shape[0]
    for k, block in enumerate(blocks):
        a_ref[k * rows : (k + 1) * rows, :] = block[:, :WA]
        b_ref[k * rows : (k + 1) * rows, :] = block[:, WA:]


def together(*values):
    return lax.optimization_barrier(values)


def ring_z(block):
    up, down = [block], [block]
    for k in range(4):
        up.append(sent(up[-1], Z_UP))
        if k < 3:
            down.append(sent(down[-1], Z_DOWN))
    return down + [up[4], up[3], up[2], up[1]]


def ring_four(block, up, down):
    below = sent(block, up)
    above = sent(block, down)
    half = block.shape[0] // 2
    return below, above, lambda: (sent(below[:half], up), sent(above[half:], down))


def layer(
    acts,
    in_proj,
    out_proj,
    conv_weight,
    conv_bias,
    dt_bias,
    decay_rate,
    skip_gain,
    level_bias,
    norm_gain,
    gate_gain,
):
    index = lax.axis_index("seq")
    y = index % NY
    z = (index // NY) % NZ
    x = index // (NY * NZ)
    w0, w1, w2, w3 = run_columns(y, in_proj[0])
    columns = run_join(y, (w0, sent(w1, Y_UP), sent(w2, Y_TWO), sent(w3, Y_DOWN)))
    tail, _ = together(acts[0, ROWS - HALO :], w1)
    halo = sent(tail, HALO_NEXT)
    order = jnp.stack([x, (x + 3) % NX, (x + 1) % NX, (x + 2) % NX, (512 - 64 * z) % 512])
    u = run_norm(order, halo, acts[0], norm_gain)

    blocks = ring_z(columns)
    u, _ = together(u, columns)
    below, above, _ = ring_four(u, Y_UP, Y_DOWN)
    lo, hi, _ = together(below[:SPLIT], above[SPLIT:], blocks[3])
    far_lo, far_hi = sent(lo, Y_UP), sent(hi, Y_DOWN)
    rows = run(
        stack_kernel, (y.reshape(1),), (u, below, above, far_lo, far_hi),
        [shape_of(BF, NY, EXT, u.shape[1])],
    )[0]
    depth = len(blocks) * blocks[0].shape[0]
    by_a, by_b = run(gather_kernel, (), blocks, [shape_of(BF, depth, WA), shape_of(BF, depth, WB)])

    y, zero, _ = together(y, jnp.zeros((), jnp.int32), blocks[7])
    piece = lambda v, width: lax.dynamic_slice_in_dim(v, y * width, width, v.ndim - 1)
    taps_a = jnp.concatenate(
        [piece(conv_weight[0, :, :2048], XW), conv_weight[0, :, 2048 : 2048 + NS]], axis=1
    )
    bias_a = jnp.concatenate(
        [piece(conv_bias[:, :2048], XW), conv_bias[:, 2048 : 2048 + NS]], axis=1
    )
    pad = jnp.zeros((1, 128 - HEADS * 9), F32)
    small_bias = jnp.concatenate(
        [piece(level_bias, HEADS * 8), piece(dt_bias, HEADS), pad], axis=1
    )
    rate = jnp.concatenate(
        [jnp.zeros((1, HEADS * 8), F32), piece(decay_rate, HEADS), pad], axis=1
    )
    skip = jnp.repeat(piece(skip_gain, HEADS), HD, axis=1)
    spreads = jnp.stack([spread(zero + k, 8) for k in range(8)] + [spread(zero + HEADS * 8, 1)])

    a_below, a_above, a_far = ring_four(by_a, X_UP, X_DOWN)
    fa_a, fb_a = a_far()
    part_a = run_part(rows, by_a, a_below, a_above)

    by_b, fa_a, fb_a = together(by_b, fa_a, fb_a)
    b_below, b_above, b_far = ring_four(by_b, X_UP, X_DOWN)
    xs, b_mat, sp, cum, e2, sc, row, states, pair, state, logs, message = run_state(
        part_a, rows, fa_a, fb_a, taps_a, bias_a, small_bias, rate, spreads
    )
    fa_b, fb_b = b_far()
    part_b = run_part(rows, by_b, b_below, b_above)

    bits = [z & 1, (z >> 1) & 1, (z >> 2) & 1, x & 1, (x >> 1) & 1]
    buckets = []
    for bit, pairs in zip(bits, EXCHANGES, strict=True):
        got = sent(message, pairs)
        message, state, logs, bucket = run_merge(bit, got, state, logs)
        buckets.append(bucket)

    y_part, c_mat, z_cols = run_intra(
        part_b, rows, fa_b, fb_b, conv_weight[0, :, 2048 + NS :], conv_bias[:, 2048 + NS :], skip,
        xs, b_mat, sp, cum, e2, row, states, pair, spreads,
    )
    block = lambda k: (y + k) % NY
    q2, q1 = run_cross((block(2), block(1)), y_part, c_mat, sc, z_cols, buckets, spreads)
    q3, q0 = run_cross((block(3), block(0)), y_part, c_mat, sc, z_cols, buckets, spreads)
    blocks = (q0, sent(q1, Y_UP), sent(q2, Y_TWO), sent(q3, Y_DOWN))
    heads_at = jnp.stack([block(0), block(3), block(2), block(1)])
    result = run_out(heads_at, blocks, gate_gain, out_proj[0], acts[0])
    return lax.ppermute(result, "section", [(0, 1), (1, 0)])[None]


def solution(mesh):
    return jax.shard_map(
        layer,
        mesh=mesh,
        in_specs=(
            P("section", "seq", None),
            P("section", "seq", None),
            P("section", None, None),
            P("section", None, None),
            P("section", None),
            P("section", None),
            P("section", None),
            P("section", None),
            P("section", None),
            P("section", None),
            P("section", None),
        ),
        out_specs=P("section", "seq", None),
        check_vma=False,
    )
```

```python
import functools

import jax
import jax.numpy as jnp
from jax import lax
from jax.experimental import pallas as pl
from jax.experimental.pallas import tpu as pltpu
from jax.sharding import PartitionSpec as P

EPS = 1e-05
F32 = jnp.float32
BF = jnp.bfloat16


NX, NZ, NY = 4, 8, 4
ROWS = 256
HEADS = 8
HD = 64
XW = HEADS * HD
NS = 128
HALO = 16
WA, WB = 768, 640
EXT = ROWS + HALO
SPLIT = 144
KX = 512


def route(move):
    pairs = []
    for x in range(NX):
        for z in range(NZ):
            for y in range(NY):
                a, b, c = move(x, z, y)
                pairs.append(
                    ((x * NZ + z) * NY + y, ((a % NX) * NZ + b % NZ) * NY + c % NY)
                )
    return pairs


X_UP = route(lambda x, z, y: (x + 1, z, y))
X_DOWN = route(lambda x, z, y: (x - 1, z, y))
Z_UP = route(lambda x, z, y: (x, z + 1, y))
Z_DOWN = route(lambda x, z, y: (x, z - 1, y))
Y_UP = route(lambda x, z, y: (x, z, y + 1))
Y_DOWN = route(lambda x, z, y: (x, z, y - 1))
Y_TWO = route(lambda x, z, y: (x, z, y + 2))
HALO_NEXT = [(i, i + 1) for i in range(NX * NZ * NY - 1)]
EXCHANGES = [
    route(lambda x, z, y: (x, z ^ 1, y)),
    route(lambda x, z, y: (x, z ^ 2, y)),
    route(lambda x, z, y: (x, 7 - z, y)),
    route(lambda x, z, y: (x ^ 1, z, y)),
    route(lambda x, z, y: (3 - x, z, y)),
]


def sent(value, pairs):
    return lax.ppermute(getattr(value, "value", value), "seq", pairs)


def spread(first, stride):
    row = lax.broadcasted_iota(jnp.int32, (128, XW), 0)
    col = lax.broadcasted_iota(jnp.int32, (128, XW), 1)
    return jnp.where(row == first + stride * (col // HD), 1.0, 0.0).astype(BF)


def mm(a, b):
    return jnp.dot(a.astype(BF), b.astype(BF), preferred_element_type=F32)


def softplus(v):
    return jnp.maximum(v, 0.0) + jnp.log1p(jnp.exp(-jnp.abs(v)))


def silu(v):
    half = 0.5 * v
    return half + half * jnp.tanh(half)


def conv_block(wide, taps, bias):
    mixed = bias[0:1, :] + taps[0:1, :] * wide[HALO - 3 : HALO - 3 + ROWS, :]
    for k in range(1, 4):
        mixed = mixed + taps[k : k + 1, :] * wide[HALO - 3 + k : HALO - 3 + k + ROWS, :]
    return silu(mixed)


def shape_of(dtype, *shape):
    return pltpu.VMEM(shape, dtype)


class Kept:
    def __init__(self, value, out):
        self.value = self.loose = value
        if out.memory_space == pltpu.HBM:
            self.value = far(value)
        self.shape = value.shape
        self.dtype = value.dtype


def plain(dtype, *shape):
    return pltpu.HBM(shape, dtype)


def near(value):
    return pltpu.with_memory_space_constraint(value, pltpu.VMEM)


def far(value):
    return pltpu.with_memory_space_constraint(value, pltpu.HBM)


def run(kernel, scalars, arrays, outs, scratch=(), place=near, loose=False):
    smem = pl.BlockSpec(memory_space=pltpu.SMEM)
    vmem = pl.BlockSpec(memory_space=pltpu.VMEM)
    kept = lambda v: v.loose if loose else v.value
    arrays = [kept(v) if isinstance(v, Kept) else place(v) for v in arrays]
    results = pl.pallas_call(
        kernel,
        in_specs=[smem] * len(scalars) + [vmem] * len(arrays),
        out_specs=[vmem] * len(outs),
        out_shape=outs,
        scratch_shapes=list(scratch),
        compiler_params=pltpu.CompilerParams(vmem_limit_bytes=10 << 20),
    )(*scalars, *arrays)
    return [Kept(v, out) for v, out in zip(results, outs, strict=True)]


def each_block(body):
    def step(j, carry):
        body(j)
        return carry

    lax.fori_loop(0, NY, step, 0)


def part_kernel(rows_ref, own_ref, below_ref, above_ref, out_ref):
    def block(j):
        total = None
        for k, w_ref in enumerate((own_ref, below_ref, above_ref)):
            there = rows_ref[j, :, k * KX : (k + 1) * KX]
            part = jnp.dot(there, w_ref[...], preferred_element_type=F32)
            total = part if total is None else total + part
        out_ref[j] = total

    each_block(block)


def run_part(rows, own, below, above, where):
    out = where(F32, NY, EXT, own.shape[1])
    return run(part_kernel, (), (rows, own, below, above), [out])[0]


def stack_kernel(y_ref, own_ref, below_ref, above_ref, lo_ref, hi_ref, near_ref, far_ref):
    y = y_ref[0]
    edge = 3 * KX
    for out_ref, a, b in ((near_ref, 0, edge), (far_ref, edge, edge + KX)):
        out_ref[y] = own_ref[:, a:b]
        out_ref[(y + 3) % NY] = below_ref[:, a:b]
        out_ref[(y + 1) % NY] = above_ref[:, a:b]
        out_ref[(y + 2) % NY, 0:SPLIT, :] = lo_ref[:, a:b]
        out_ref[(y + 2) % NY, SPLIT:, :] = hi_ref[:, a:b]


def finished(part_ref, rows_ref, fa_ref, fb_ref, j):
    total = (
        part_ref[j]
        + jnp.dot(rows_ref[j, :, : KX // 2], fa_ref[...], preferred_element_type=F32)
        + jnp.dot(rows_ref[j, :, KX // 2 :], fb_ref[...], preferred_element_type=F32)
    )
    return total.astype(BF).astype(F32)


def state_kernel(
    part_ref, rows_ref, fa_ref, fb_ref, taps_ref, bias_ref, small_bias_ref, rate_ref, spread_ref,
    xs_ref, b_ref, sp_ref, cum_ref, e2_ref, sc_ref, row_ref, s_ref, pair_ref, logs_ref, msg_ref,
    wide_ref, acc_ref, carry_ref,
):
    acc_ref[...] = jnp.zeros_like(acc_ref)
    carry_ref[...] = jnp.zeros_like(carry_ref)
    logs_ref[...] = jnp.zeros_like(logs_ref)

    def block(j):
        p = finished(part_ref, rows_ref, fa_ref, fb_ref, j)
        wide_ref[...] = p[:, : XW + NS]
        mixed = conv_block(wide_ref, taps_ref, bias_ref)
        xs = mixed[:, :XW]
        b_mat = mixed[:, XW:]
        sp = softplus(p[HALO:, XW + NS :] + small_bias_ref[0:1, :])
        g = -sp * rate_ref[0:1, :]
        row = lax.broadcasted_iota(jnp.int32, (ROWS, ROWS), 0)
        col = lax.broadcasted_iota(jnp.int32, (ROWS, ROWS), 1)
        tri = jnp.where(col <= row, 1.0, 0.0).astype(BF)
        g0 = g.astype(BF)
        r1 = g - g0.astype(F32)
        g1 = r1.astype(BF)
        g2 = r1 - g1.astype(F32)
        cum = mm(tri, g0) + mm(tri, g1) + mm(tri, g2)
        last = cum[ROWS - 1 : ROWS, :]
        tail = jnp.exp(last - cum) * sp
        head_spread = spread_ref[8]
        xt = xs * mm(tail, head_spread)
        state = mm(b_mat.T, xt)
        last8 = jnp.broadcast_to(last, (16, 128))
        hi = last8.astype(BF)
        rest = last8 - hi.astype(F32)
        mid = rest.astype(BF)
        low = rest - mid.astype(F32)
        last_wide = mm(hi, head_spread) + mm(mid, head_spread) + mm(low, head_spread)
        acc = jnp.exp(last_wide[0:1, :]) * acc_ref[...] + state
        acc_ref[...] = acc
        group = carry_ref[0:1, :]
        pair = jnp.where(j == 2, 0.0, carry_ref[1:2, :])
        e2_ref[j] = jnp.exp(cum + pair)
        lane = lax.broadcasted_iota(jnp.int32, (128, 128), 1)
        src = lax.broadcasted_iota(jnp.int32, (128, 128), 0)
        to_levels = jnp.where(src - HEADS * 8 == lane // 8, 1.0, 0.0)
        sc_ref[j] = (sp * mm(jnp.exp(cum + group), to_levels)).astype(BF)
        carry_ref[0:1, :] = group + last
        carry_ref[1:2, :] = pair + last
        xs_ref[j] = xs
        b_ref[j] = b_mat.astype(BF)
        sp_ref[j] = sp
        cum_ref[j] = cum
        row_ref[j] = cum.T[HEADS * 8 : HEADS * 9, :]
        s_ref[j] = state.astype(BF)
        logs_ref[0:1, :] = logs_ref[0:1, :] + last_wide[0:1, :]

        @pl.when(j == 1)
        def _():
            pair_ref[...] = acc.astype(BF)

        @pl.when(j == NY - 1)
        def _():
            pack_message(msg_ref, acc, logs_ref[0:1, :])

    each_block(block)


def pack_message(msg_ref, state, log):
    msg_ref[0:NS, :] = state.astype(BF)
    hi = log.astype(BF).astype(F32)
    row = lax.broadcasted_iota(jnp.int32, (16, XW), 0)
    both = jnp.where(row == 0, hi, jnp.where(row == 1, log - hi, 0.0))
    msg_ref[NS:, :] = both.astype(BF)


def run_state(part, rows, far_a, far_b, taps, bias, small_bias, rate, spreads):
    return run(
        state_kernel,
        (),
        (part, rows, far_a, far_b, taps, bias, small_bias, rate, spreads),
        [
            plain(F32, NY, ROWS, XW), plain(BF, NY, ROWS, NS), plain(F32, NY, ROWS, 128),
            plain(F32, NY, ROWS, 128), plain(F32, NY, ROWS, 128), plain(BF, NY, ROWS, 128),
            plain(F32, NY, HEADS, ROWS), plain(BF, NY, NS, XW),
            plain(BF, NS, XW), shape_of(F32, 16, XW), shape_of(BF, NS + 16, XW),
        ],
        [
            pltpu.VMEM((EXT, XW + NS), F32),
            pltpu.VMEM((NS, XW), F32),
            pltpu.VMEM((8, 128), F32),
        ],
    )


def intra_kernel(
    part_ref, rows_ref, fa_ref, fb_ref, taps_ref, bias_ref, skip_ref,
    xs_ref, b_ref, sp_ref, cum_ref, e2_ref, row_ref, s1_ref, s2_ref, spread_ref,
    y_ref, c_ref, z_ref, wide_ref,
):
    def block(j):
        p = finished(part_ref, rows_ref, fa_ref, fb_ref, j)
        z_ref[j] = p[HALO:, :XW].astype(BF)
        wide_ref[...] = p[:, XW:]
        c_mat = conv_block(wide_ref, taps_ref, bias_ref).astype(BF)
        c_ref[j] = c_mat
        xs = xs_ref[j]
        sp = sp_ref[j].astype(BF)
        cum = cum_ref[j]
        scores = lax.dot_general(
            c_mat, b_ref[j], (((1,), (1,)), ((), ())), preferred_element_type=F32
        )
        row = lax.broadcasted_iota(jnp.int32, (ROWS, ROWS), 0)
        col = lax.broadcasted_iota(jnp.int32, (ROWS, ROWS), 1)
        causal = col <= row
        head_spread = spread_ref[8]
        xd = (xs * mm(sp, head_spread)).astype(BF)
        parts = []
        for h in range(HEADS):
            lane = HEADS * 8 + h
            diff = cum[:, lane : lane + 1] - row_ref[j, h : h + 1, :]
            decay = jnp.exp(jnp.where(causal, diff, -1e30)) * scores
            parts.append(mm(decay, xd[:, h * HD : (h + 1) * HD]))
        y = jnp.concatenate(parts, axis=1) * mm(sp, spread_ref[0])
        y = y + skip_ref[0:1, :] * xs
        odd = (j % 2).astype(F32)
        late = (j // 2).astype(F32)
        one = mm(sp, spread_ref[1]) * mm(jnp.exp(cum), head_spread)
        y = y + mm(c_mat, s1_ref[(j // 2) * 2]) * (one * odd)
        two = mm(sp, spread_ref[2]) * mm(e2_ref[j], head_spread)
        y = y + mm(c_mat, s2_ref[...]) * (two * late)
        y_ref[j] = y

    each_block(block)


def run_intra(part, rows, far_a, far_b, taps, bias, skip, xs, b_mat, sp, cum, e2, row, states, pair, spreads):
    return run(
        intra_kernel,
        (),
        (part, rows, far_a, far_b, taps, bias, skip, xs, b_mat, sp, cum, e2, row, states, pair, spreads),
        [plain(F32, NY, ROWS, XW), plain(BF, NY, ROWS, NS), plain(BF, NY, ROWS, XW)],
        [pltpu.VMEM((EXT, NS), F32)],
        place=lambda v: v,
        loose=True,
    )


def merge_kernel(mask_ref, got_ref, own_ref, logs_ref, msg_ref, new_logs_ref, *, k):
    upper = mask_ref[k : k + 1, :] == 1
    other = got_ref[0:NS, :].astype(F32)
    tail = got_ref[NS:, :].astype(F32)
    other_log = tail[0:1, :] + tail[1:2, :]
    log = logs_ref[0:1, :]
    before = logs_ref[1:2, :]
    state = (
        jnp.where(upper, jnp.exp(log), 1.0) * other
        + jnp.where(upper, 1.0, jnp.exp(other_log)) * own_ref[0:NS, :].astype(F32)
    )
    log = log + other_log
    new_logs_ref[...] = logs_ref[...]
    new_logs_ref[0:1, :] = log
    new_logs_ref[1:2, :] = jnp.where(upper, before + other_log, before)
    new_logs_ref[8 + k : 9 + k, :] = jnp.where(upper, jnp.exp(before), 0.0)
    pack_message(msg_ref, state, log)


def run_merge(k, masks, got, own, logs):
    return run(
        functools.partial(merge_kernel, k=k),
        (),
        (masks, got, own, logs),
        [shape_of(BF, NS + 16, XW), shape_of(F32, 16, XW)],
    )


def cross_kernel(
    at_ref, y_ref, c_ref, sc_ref, z_ref, g3, g4, g5, g6, g7, logs_ref, spread_ref,
    q0, q1, q2, q3, bucket_ref,
):
    for k, got in enumerate((g3, g4, g5, g6, g7)):
        scaled = got[0:NS, :].astype(F32) * logs_ref[8 + k : 9 + k, :]
        bucket_ref[k] = scaled.astype(BF)
    for k, q_ref in enumerate((q0, q1, q2, q3)):
        j = at_ref[k]
        c_mat = c_ref[j]
        scale = sc_ref[j]
        y = y_ref[j]
        for level in range(3, 8):
            y = y + mm(c_mat, bucket_ref[level - 3]) * mm(scale, spread_ref[level])
        q_ref[...] = (y * silu(z_ref[j].astype(F32))).astype(BF)


def run_cross(at, y, c_mat, sc, z, gots, logs, spreads):
    return run(
        cross_kernel,
        (at,),
        (y, c_mat, sc, z, *gots, logs, spreads),
        [shape_of(BF, ROWS, XW)] * NY,
        [pltpu.VMEM((5, NS, XW), BF)],
        place=lambda v: v,
    )


def out_kernel(at_ref, q0, q1, q2, q3, gain_ref, acts_ref, w_ref, out_ref, acc_ref, w_vmem, sems):
    blocks = (q0, q1, q2, q3)
    rows = [pl.ds(pl.multiple_of(at_ref[k] * XW, XW), XW) for k in range(NY)]
    copies = [
        pltpu.make_async_copy(w_ref.at[rows[k], :], w_vmem.at[k], sems.at[k]) for k in range(NY)
    ]
    for copy in copies:
        copy.start()
    square = sum(
        jnp.sum(jnp.square(q[...].astype(F32)), axis=1, keepdims=True) for q in blocks
    )
    scale = lax.rsqrt(square / (NY * XW) + EPS)
    acc_ref[...] = acts_ref[...].astype(F32)
    for k, q in enumerate(blocks):
        n = q[...].astype(F32) * scale * gain_ref[0:1, rows[k]]
        copies[k].wait()
        acc_ref[...] += jnp.dot(n.astype(BF), w_vmem[k], preferred_element_type=F32)
    out_ref[...] = acc_ref[...].astype(BF)


def run_out(at, blocks, gain, weight, acts):
    width = weight.shape[1]
    vmem = pl.BlockSpec(memory_space=pltpu.VMEM)
    blocks = [v.value if isinstance(v, Kept) else near(v) for v in blocks]
    return pl.pallas_call(
        out_kernel,
        in_specs=[pl.BlockSpec(memory_space=pltpu.SMEM)]
        + [vmem] * 6
        + [pl.BlockSpec(memory_space=pltpu.HBM)],
        out_specs=vmem,
        out_shape=shape_of(BF, ROWS, width),
        scratch_shapes=[
            pltpu.VMEM((ROWS, width), F32),
            pltpu.VMEM((NY, XW, width), BF),
            pltpu.SemaphoreType.DMA((NY,)),
        ],
        compiler_params=pltpu.CompilerParams(vmem_limit_bytes=28 << 20),
        name="gate_out",
    )(at, *blocks, gain, acts, far(weight))


def norm_kernel(at_ref, halo_ref, acts_ref, gain_ref, out_ref, full_ref):
    for start, ref in ((0, halo_ref), (HALO, acts_ref)):
        v = ref[...].astype(F32)
        scale = lax.rsqrt(jnp.mean(v * v, axis=1, keepdims=True) + EPS)
        full_ref[start : start + v.shape[0], :] = v * scale * gain_ref[0:1, :]
    for k in range(NX):
        start = pl.multiple_of(at_ref[k] * KX, KX)
        part = pltpu.roll(full_ref[:, pl.ds(start, KX)], at_ref[NX], 1)
        out_ref[:, k * KX : (k + 1) * KX] = part.astype(BF)


def run_norm(at, halo, acts, gain):
    width = acts.shape[1]
    return run(
        norm_kernel,
        (at,),
        (halo, acts, gain),
        [shape_of(BF, EXT, width)],
        [pltpu.VMEM((EXT, width), F32)],
        place=lambda v: v,
    )[0]


def columns_kernel(y_ref, shard_ref, o0, o1, o2, o3, all_ref):
    shard = shard_ref[...]
    for t in range(NY):
        x0, z0 = t * XW, 2304 + t * XW
        dt0, lv0 = 4352 + t * HEADS, 4384 + t * HEADS * 8
        all_ref[t, :, 0:XW] = shard[:, x0 : x0 + XW]
        all_ref[t, :, XW : XW + NS] = shard[:, 2048 : 2048 + NS]
        all_ref[t, :, XW + NS : WA] = jnp.concatenate(
            [
                shard[:, lv0 : lv0 + HEADS * 8].astype(F32),
                shard[:, dt0 : dt0 + HEADS].astype(F32),
                jnp.zeros((shard.shape[0], 128 - HEADS * 9), F32),
            ],
            axis=1,
        ).astype(BF)
        all_ref[t, :, WA : WA + XW] = shard[:, z0 : z0 + XW]
        all_ref[t, :, WA + XW :] = shard[:, 2048 + NS : 2304]
    for k, out in enumerate((o0, o1, o2, o3)):
        out[...] = all_ref[(y_ref[0] + k) % NY]


def run_columns(y, shard):
    rows = shard.shape[0]
    return run(
        columns_kernel,
        (y.reshape(1),),
        (shard,),
        [shape_of(BF, rows, WA + WB)] * 4,
        [pltpu.VMEM((NY, rows, WA + WB), BF)],
        place=lambda v: v,
    )


def join_kernel(y_ref, b0, b1, b2, b3, out_ref):
    rows = b0.shape[0]
    for back, block in ((0, b0), (3, b1), (2, b2), (1, b3)):
        start = pl.multiple_of(((y_ref[0] + back) % NY) * rows, rows)
        out_ref[pl.ds(start, rows), :] = block[...]


def run_join(y, blocks):
    rows, width = blocks[0].shape
    return run(join_kernel, (y.reshape(1),), blocks, [shape_of(BF, NY * rows, width)])[0]


def gather_kernel(*refs):
    *blocks, a_ref, b_ref = refs
    rows = blocks[0].shape[0]
    for k, block in enumerate(blocks):
        a_ref[k * rows : (k + 1) * rows, :] = block[:, :WA]
        b_ref[k * rows : (k + 1) * rows, :] = block[:, WA:]


def together(*values):
    return lax.optimization_barrier(values)


def ring_z(block):
    up, down = [block], [block]
    for k in range(4):
        up.append(sent(up[-1], Z_UP))
        if k < 3:
            down.append(sent(down[-1], Z_DOWN))
    return down + [up[4], up[3], up[2], up[1]]


def half_kernel(block_ref, out_ref, *, start):
    out_ref[...] = block_ref[start : start + out_ref.shape[0], :]


def rows_from(block, start, count):
    kernel = functools.partial(half_kernel, start=start)
    return run(kernel, (), (block,), [shape_of(BF, count, block.shape[1])])[0]


def near_pair(block, up, down):
    return sent(block, up), sent(block, down)


def far_pair(below, above, up, down, split):
    rest = above.shape[0] - split
    return sent(rows_from(below, 0, split), up), sent(rows_from(above, split, rest), down)


def mask_kernel(bits_ref, out_ref):
    for k in range(8):
        out_ref[k : k + 1, :] = jnp.full((1, XW), bits_ref[k], jnp.int32)


def layer(
    acts,
    in_proj,
    out_proj,
    conv_weight,
    conv_bias,
    dt_bias,
    decay_rate,
    skip_gain,
    level_bias,
    norm_gain,
    gate_gain,
):
    index = lax.axis_index("seq")
    y = index % NY
    z = (index // NY) % NZ
    x = index // (NY * NZ)
    w0, w1, w2, w3 = run_columns(y, in_proj[0])
    shared = (w0, sent(w1, Y_UP), sent(w2, Y_TWO), sent(w3, Y_DOWN))
    columns = run_join(y, shared)
    halo = sent(acts[0, ROWS - HALO :], HALO_NEXT)
    order = jnp.stack([x, (x + 3) % NX, (x + 1) % NX, (x + 2) % NX, (512 - 64 * z) % 512])
    u = run_norm(order, halo, acts[0], norm_gain)

    blocks = ring_z(columns)
    below, above = near_pair(u, Y_UP, Y_DOWN)
    far_lo, far_hi = far_pair(below, above, Y_UP, Y_DOWN, SPLIT)
    rows, rows_far = run(
        stack_kernel, (y.reshape(1),), (u, below, above, far_lo, far_hi),
        [plain(BF, NY, EXT, 3 * KX), plain(BF, NY, EXT, KX)],
    )
    depth = len(blocks) * blocks[1].shape[0]
    by_a, by_b = run(gather_kernel, (), blocks, [shape_of(BF, depth, WA), plain(BF, depth, WB)])

    y, zero, _ = together(y, jnp.zeros((), jnp.int32), blocks[7])
    piece = lambda v, width: lax.dynamic_slice_in_dim(v, y * width, width, v.ndim - 1)
    taps_a = jnp.concatenate(
        [piece(conv_weight[0, :, :2048], XW), conv_weight[0, :, 2048 : 2048 + NS]], axis=1
    )
    bias_a = jnp.concatenate(
        [piece(conv_bias[:, :2048], XW), conv_bias[:, 2048 : 2048 + NS]], axis=1
    )
    pad = jnp.zeros((1, 128 - HEADS * 9), F32)
    small_bias = jnp.concatenate(
        [piece(level_bias, HEADS * 8), piece(dt_bias, HEADS), pad], axis=1
    )
    rate = jnp.concatenate(
        [jnp.zeros((1, HEADS * 8), F32), piece(decay_rate, HEADS), pad], axis=1
    )
    skip = jnp.repeat(piece(skip_gain, HEADS), HD, axis=1)
    spreads = jnp.stack([spread(zero + k, 8) for k in range(8)] + [spread(zero + HEADS * 8, 1)])

    bits = jnp.stack([z & 1, (z >> 1) & 1, (z >> 2) & 1, x & 1, (x >> 1) & 1, zero, zero, zero])
    masks = run(mask_kernel, (bits,), (), [shape_of(jnp.int32, 8, XW)])[0]

    a_below, a_above = near_pair(by_a, X_UP, X_DOWN)
    fa_a, fb_a = far_pair(a_below, a_above, X_UP, X_DOWN, KX // 2)
    part_a = run_part(rows, by_a, a_below, a_above, shape_of)

    b_below, b_above = near_pair(by_b, X_UP, X_DOWN)
    xs, b_mat, sp, cum, e2, sc, row, states, pair, logs, message = run_state(
        part_a, rows_far, fa_a, fb_a, taps_a, bias_a, small_bias, rate, spreads
    )
    fa_b, fb_b = far_pair(b_below, b_above, X_UP, X_DOWN, KX // 2)
    part_b = run_part(rows, by_b, b_below, b_above, plain)

    gots = []
    for k, pairs in enumerate(EXCHANGES):
        got = sent(message, pairs)
        message, logs = run_merge(k, masks, got, message, logs)
        gots.append(got)

    y_part, c_mat, z_cols = run_intra(
        part_b, rows_far, fa_b, fb_b, conv_weight[0, :, 2048 + NS :], conv_bias[:, 2048 + NS :], skip,
        xs, b_mat, sp, cum, e2, row, states, pair, spreads,
    )
    block = lambda k: (y + k) % NY
    order = jnp.stack([block(k) for k in range(NY)])
    q0, q1, q2, q3 = run_cross(order, y_part, c_mat, sc, z_cols, gots, logs, spreads)
    blocks = (q0, sent(q1, Y_UP), sent(q2, Y_TWO), sent(q3, Y_DOWN))
    heads_at = jnp.stack([block(0), block(3), block(2), block(1)])
    result = run_out(heads_at, blocks, gate_gain, out_proj[0], acts[0])
    return lax.ppermute(result, "section", [(0, 1), (1, 0)])[None]


def solution(mesh):
    return jax.shard_map(
        layer,
        mesh=mesh,
        in_specs=(
            P("section", "seq", None),
            P("section", "seq", None),
            P("section", None, None),
            P("section", None, None),
            P("section", None),
            P("section", None),
            P("section", None),
            P("section", None),
            P("section", None),
            P("section", None),
            P("section", None),
        ),
        out_specs=P("section", "seq", None),
        check_vma=False,
    )
```

```python
import functools

import jax
import jax.numpy as jnp
from jax import lax
from jax.experimental import pallas as pl
from jax.experimental.pallas import tpu as pltpu
from jax.sharding import PartitionSpec as P

EPS = 1e-05
F32 = jnp.float32
BF = jnp.bfloat16


NX, NZ, NY = 4, 8, 4
ROWS = 256
HEADS = 8
HD = 64
XW = HEADS * HD
NS = 128
HALO = 16
WA, WB = 768, 640
EXT = ROWS + HALO
SPLIT = 144
KX = 512


def route(move):
    pairs = []
    for x in range(NX):
        for z in range(NZ):
            for y in range(NY):
                a, b, c = move(x, z, y)
                pairs.append(
                    ((x * NZ + z) * NY + y, ((a % NX) * NZ + b % NZ) * NY + c % NY)
                )
    return pairs


X_UP = route(lambda x, z, y: (x + 1, z, y))
X_DOWN = route(lambda x, z, y: (x - 1, z, y))
X_TWO = route(lambda x, z, y: (x + 2, z, y))
Z_UP = route(lambda x, z, y: (x, z + 1, y))
Z_DOWN = route(lambda x, z, y: (x, z - 1, y))
Y_UP = route(lambda x, z, y: (x, z, y + 1))
Y_DOWN = route(lambda x, z, y: (x, z, y - 1))
Y_TWO = route(lambda x, z, y: (x, z, y + 2))
HALO_NEXT = [(i, i + 1) for i in range(NX * NZ * NY - 1)]
EXCHANGES = [
    route(lambda x, z, y: (x, z ^ 1, y)),
    route(lambda x, z, y: (x, z ^ 2, y)),
    route(lambda x, z, y: (x, 7 - z, y)),
    route(lambda x, z, y: (x ^ 1, z, y)),
    route(lambda x, z, y: (3 - x, z, y)),
]


def sent(value, pairs):
    return lax.ppermute(getattr(value, "value", value), "seq", pairs)


def spread(first, stride):
    row = lax.broadcasted_iota(jnp.int32, (128, XW), 0)
    col = lax.broadcasted_iota(jnp.int32, (128, XW), 1)
    return jnp.where(row == first + stride * (col // HD), 1.0, 0.0).astype(BF)


def mm(a, b):
    return jnp.dot(a.astype(BF), b.astype(BF), preferred_element_type=F32)


def softplus(v):
    return jnp.maximum(v, 0.0) + jnp.log1p(jnp.exp(-jnp.abs(v)))


def silu(v):
    half = 0.5 * v
    return half + half * jnp.tanh(half)


def conv_block(wide, taps, bias):
    mixed = bias[0:1, :] + taps[0:1, :] * wide[HALO - 3 : HALO - 3 + ROWS, :]
    for k in range(1, 4):
        mixed = mixed + taps[k : k + 1, :] * wide[HALO - 3 + k : HALO - 3 + k + ROWS, :]
    return silu(mixed)


def shape_of(dtype, *shape):
    return pltpu.VMEM(shape, dtype)


class Kept:
    def __init__(self, value, out):
        self.value = self.loose = value
        if out.memory_space == pltpu.HBM:
            self.value = far(value)
        self.shape = value.shape
        self.dtype = value.dtype


def plain(dtype, *shape):
    return pltpu.HBM(shape, dtype)


def near(value):
    return pltpu.with_memory_space_constraint(value, pltpu.VMEM)


def far(value):
    return pltpu.with_memory_space_constraint(value, pltpu.HBM)


def run(kernel, scalars, arrays, outs, scratch=(), place=near, loose=False):
    smem = pl.BlockSpec(memory_space=pltpu.SMEM)
    vmem = pl.BlockSpec(memory_space=pltpu.VMEM)
    kept = lambda v: v.loose if loose else v.value
    arrays = [kept(v) if isinstance(v, Kept) else place(v) for v in arrays]
    results = pl.pallas_call(
        kernel,
        in_specs=[smem] * len(scalars) + [vmem] * len(arrays),
        out_specs=[vmem] * len(outs),
        out_shape=outs,
        scratch_shapes=list(scratch),
        compiler_params=pltpu.CompilerParams(vmem_limit_bytes=10 << 20),
    )(*scalars, *arrays)
    return [Kept(v, out) for v, out in zip(results, outs, strict=True)]


def each_block(body):
    def step(j, carry):
        body(j)
        return carry

    lax.fori_loop(0, NY, step, 0)


def part_kernel(rows_ref, own_ref, below_ref, above_ref, out_ref):
    def block(j):
        total = None
        for k, w_ref in enumerate((own_ref, below_ref, above_ref)):
            there = rows_ref[j, :, k * KX : (k + 1) * KX]
            part = jnp.dot(there, w_ref[...], preferred_element_type=F32)
            total = part if total is None else total + part
        out_ref[j] = total

    each_block(block)


def run_part(rows, own, below, above, where):
    out = where(F32, NY, EXT, own.shape[1])
    return run(part_kernel, (), (rows, own, below, above), [out])[0]


def stack_kernel(y_ref, own_ref, below_ref, above_ref, lo_ref, hi_ref, near_ref, far_ref):
    y = y_ref[0]
    edge = 3 * KX
    for out_ref, a, b in ((near_ref, 0, edge), (far_ref, edge, edge + KX)):
        out_ref[y] = own_ref[:, a:b]
        out_ref[(y + 3) % NY] = below_ref[:, a:b]
        out_ref[(y + 1) % NY] = above_ref[:, a:b]
        out_ref[(y + 2) % NY, 0:SPLIT, :] = lo_ref[:, a:b]
        out_ref[(y + 2) % NY, SPLIT:, :] = hi_ref[:, a:b]


def finished(part_ref, rows_ref, fa_ref, fb_ref, j):
    total = (
        part_ref[j]
        + jnp.dot(rows_ref[j, :, : KX // 2], fa_ref[...], preferred_element_type=F32)
        + jnp.dot(rows_ref[j, :, KX // 2 :], fb_ref[...], preferred_element_type=F32)
    )
    return total.astype(BF).astype(F32)


def state_kernel(
    part_ref, rows_ref, fa_ref, fb_ref, taps_ref, bias_ref, small_bias_ref, rate_ref, spread_ref,
    xs_ref, b_ref, sp_ref, cum_ref, e2_ref, sc_ref, row_ref, s_ref, pair_ref, logs_ref, msg_ref,
    wide_ref, acc_ref, carry_ref,
):
    acc_ref[...] = jnp.zeros_like(acc_ref)
    carry_ref[...] = jnp.zeros_like(carry_ref)
    logs_ref[...] = jnp.zeros_like(logs_ref)

    def block(j):
        p = finished(part_ref, rows_ref, fa_ref, fb_ref, j)
        wide_ref[...] = p[:, : XW + NS]
        mixed = conv_block(wide_ref, taps_ref, bias_ref)
        xs = mixed[:, :XW]
        b_mat = mixed[:, XW:]
        sp = softplus(p[HALO:, XW + NS :] + small_bias_ref[0:1, :])
        g = -sp * rate_ref[0:1, :]
        row = lax.broadcasted_iota(jnp.int32, (ROWS, ROWS), 0)
        col = lax.broadcasted_iota(jnp.int32, (ROWS, ROWS), 1)
        tri = jnp.where(col <= row, 1.0, 0.0).astype(BF)
        g0 = g.astype(BF)
        r1 = g - g0.astype(F32)
        g1 = r1.astype(BF)
        g2 = r1 - g1.astype(F32)
        cum = mm(tri, g0) + mm(tri, g1) + mm(tri, g2)
        last = cum[ROWS - 1 : ROWS, :]
        tail = jnp.exp(last - cum) * sp
        head_spread = spread_ref[8]
        xt = xs * mm(tail, head_spread)
        state = mm(b_mat.T, xt)
        last8 = jnp.broadcast_to(last, (16, 128))
        hi = last8.astype(BF)
        rest = last8 - hi.astype(F32)
        mid = rest.astype(BF)
        low = rest - mid.astype(F32)
        last_wide = mm(hi, head_spread) + mm(mid, head_spread) + mm(low, head_spread)
        acc = jnp.exp(last_wide[0:1, :]) * acc_ref[...] + state
        acc_ref[...] = acc
        group = carry_ref[0:1, :]
        pair = jnp.where(j == 2, 0.0, carry_ref[1:2, :])
        e2_ref[j] = jnp.exp(cum + pair)
        lane = lax.broadcasted_iota(jnp.int32, (128, 128), 1)
        src = lax.broadcasted_iota(jnp.int32, (128, 128), 0)
        to_levels = jnp.where(src - HEADS * 8 == lane // 8, 1.0, 0.0)
        sc_ref[j] = (sp * mm(jnp.exp(cum + group), to_levels)).astype(BF)
        carry_ref[0:1, :] = group + last
        carry_ref[1:2, :] = pair + last
        xs_ref[j] = xs
        b_ref[j] = b_mat.astype(BF)
        sp_ref[j] = sp
        cum_ref[j] = cum
        row_ref[j] = cum.T[HEADS * 8 : HEADS * 9, :]
        s_ref[j] = state.astype(BF)
        logs_ref[0:1, :] = logs_ref[0:1, :] + last_wide[0:1, :]

        @pl.when(j == 1)
        def _():
            pair_ref[...] = acc.astype(BF)

        @pl.when(j == NY - 1)
        def _():
            pack_message(msg_ref, acc, logs_ref[0:1, :])

    each_block(block)


def pack_message(msg_ref, state, log):
    msg_ref[0:NS, :] = state.astype(BF)
    hi = log.astype(BF).astype(F32)
    row = lax.broadcasted_iota(jnp.int32, (16, XW), 0)
    both = jnp.where(row == 0, hi, jnp.where(row == 1, log - hi, 0.0))
    msg_ref[NS:, :] = both.astype(BF)


def run_state(part, rows, far_a, far_b, taps, bias, small_bias, rate, spreads):
    return run(
        state_kernel,
        (),
        (part, rows, far_a, far_b, taps, bias, small_bias, rate, spreads),
        [
            plain(F32, NY, ROWS, XW), plain(BF, NY, ROWS, NS), plain(F32, NY, ROWS, 128),
            plain(F32, NY, ROWS, 128), plain(F32, NY, ROWS, 128), plain(BF, NY, ROWS, 128),
            plain(F32, NY, HEADS, ROWS), plain(BF, NY, NS, XW),
            plain(BF, NS, XW), shape_of(F32, 16, XW), shape_of(BF, NS + 16, XW),
        ],
        [
            pltpu.VMEM((EXT, XW + NS), F32),
            pltpu.VMEM((NS, XW), F32),
            pltpu.VMEM((8, 128), F32),
        ],
    )


def intra_kernel(
    part_ref, rows_ref, far_ref, taps_ref, bias_ref, skip_ref,
    xs_ref, b_ref, sp_ref, cum_ref, e2_ref, row_ref, s1_ref, s2_ref, spread_ref,
    y_ref, c_ref, z_ref, wide_ref,
):
    j = pl.program_id(0)
    p = part_ref[0] + jnp.dot(rows_ref[0], far_ref[...], preferred_element_type=F32)
    p = p.astype(BF).astype(F32)
    z_ref[0] = p[HALO:, :XW].astype(BF)
    wide_ref[...] = p[:, XW:]
    c_mat = conv_block(wide_ref, taps_ref, bias_ref).astype(BF)
    c_ref[0] = c_mat
    xs = xs_ref[0]
    sp = sp_ref[0].astype(BF)
    cum = cum_ref[0]
    scores = lax.dot_general(
        c_mat, b_ref[0], (((1,), (1,)), ((), ())), preferred_element_type=F32
    )
    row = lax.broadcasted_iota(jnp.int32, (ROWS, ROWS), 0)
    col = lax.broadcasted_iota(jnp.int32, (ROWS, ROWS), 1)
    causal = col <= row
    head_spread = spread_ref[8]
    xd = (xs * mm(sp, head_spread)).astype(BF)
    parts = []
    for h in range(HEADS):
        lane = HEADS * 8 + h
        diff = cum[:, lane : lane + 1] - row_ref[0, h : h + 1, :]
        decay = jnp.exp(jnp.where(causal, diff, -1e30)) * scores
        parts.append(mm(decay, xd[:, h * HD : (h + 1) * HD]))
    y = jnp.concatenate(parts, axis=1) * mm(sp, spread_ref[0])
    y = y + skip_ref[0:1, :] * xs
    odd = (j % 2).astype(F32)
    late = (j // 2).astype(F32)
    one = mm(sp, spread_ref[1]) * mm(jnp.exp(cum), head_spread)
    y = y + mm(c_mat, s1_ref[0]) * (one * odd)
    two = mm(sp, spread_ref[2]) * mm(e2_ref[0], head_spread)
    y = y + mm(c_mat, s2_ref[...]) * (two * late)
    y_ref[0] = y


def run_intra(part, rows, w_far, taps, bias, skip, xs, b_mat, sp, cum, e2, row, states, pair, spreads):
    whole = lambda *shape: pl.BlockSpec(shape, lambda j: (0,) * len(shape))
    each = lambda a, b: pl.BlockSpec((1, a, b), lambda j: (j, 0, 0))
    arrays = (part, rows, w_far, taps, bias, skip, xs, b_mat, sp, cum, e2, row, states, pair, spreads)
    arrays = [v.value if isinstance(v, Kept) else far(v) for v in arrays]
    outs = [plain(F32, NY, ROWS, XW), plain(BF, NY, ROWS, NS), plain(BF, NY, ROWS, XW)]
    results = pl.pallas_call(
        intra_kernel,
        grid=(NY,),
        in_specs=[
            each(EXT, WB), each(EXT, KX), whole(KX, WB),
            whole(4, NS), whole(1, NS), whole(1, XW),
            each(ROWS, XW), each(ROWS, NS), each(ROWS, 128), each(ROWS, 128), each(ROWS, 128),
            each(HEADS, ROWS),
            pl.BlockSpec((1, NS, XW), lambda j: ((j // 2) * 2, 0, 0)),
            whole(NS, XW), whole(9, 128, XW),
        ],
        out_specs=[each(ROWS, XW), each(ROWS, NS), each(ROWS, XW)],
        out_shape=outs,
        scratch_shapes=[pltpu.VMEM((EXT, NS), F32)],
        compiler_params=pltpu.CompilerParams(vmem_limit_bytes=28 << 20),
        name="intra_block",
    )(*arrays)
    return [Kept(v, out) for v, out in zip(results, outs, strict=True)]


def merge_kernel(mask_ref, got_ref, own_ref, logs_ref, msg_ref, new_logs_ref, *, k):
    upper = mask_ref[k : k + 1, :] == 1
    other = got_ref[0:NS, :].astype(F32)
    tail = got_ref[NS:, :].astype(F32)
    other_log = tail[0:1, :] + tail[1:2, :]
    log = logs_ref[0:1, :]
    before = logs_ref[1:2, :]
    state = (
        jnp.where(upper, jnp.exp(log), 1.0) * other
        + jnp.where(upper, 1.0, jnp.exp(other_log)) * own_ref[0:NS, :].astype(F32)
    )
    log = log + other_log
    new_logs_ref[...] = logs_ref[...]
    new_logs_ref[0:1, :] = log
    new_logs_ref[1:2, :] = jnp.where(upper, before + other_log, before)
    new_logs_ref[8 + k : 9 + k, :] = jnp.where(upper, jnp.exp(before), 0.0)
    pack_message(msg_ref, state, log)


def run_merge(k, masks, got, own, logs):
    return run(
        functools.partial(merge_kernel, k=k),
        (),
        (masks, got, own, logs),
        [shape_of(BF, NS + 16, XW), shape_of(F32, 16, XW)],
    )


def cross_kernel(
    at_ref, y_ref, c_ref, sc_ref, z_ref, g3, g4, g5, g6, g7, logs_ref, spread_ref,
    q0, q1, q2, q3, bucket_ref,
):
    for k, got in enumerate((g3, g4, g5, g6, g7)):
        scaled = got[0:NS, :].astype(F32) * logs_ref[8 + k : 9 + k, :]
        bucket_ref[k] = scaled.astype(BF)
    for k, q_ref in enumerate((q0, q1, q2, q3)):
        j = at_ref[k]
        c_mat = c_ref[j]
        scale = sc_ref[j]
        y = y_ref[j]
        for level in range(3, 8):
            y = y + mm(c_mat, bucket_ref[level - 3]) * mm(scale, spread_ref[level])
        q_ref[...] = (y * silu(z_ref[j].astype(F32))).astype(BF)


def run_cross(at, y, c_mat, sc, z, gots, logs, spreads):
    return run(
        cross_kernel,
        (at,),
        (y, c_mat, sc, z, *gots, logs, spreads),
        [shape_of(BF, ROWS, XW)] * NY,
        [pltpu.VMEM((5, NS, XW), BF)],
        place=lambda v: v,
    )


def out_kernel(at_ref, q0, q1, q2, q3, gain_ref, acts_ref, w_ref, out_ref, acc_ref, w_vmem, sems):
    blocks = (q0, q1, q2, q3)
    rows = [pl.ds(pl.multiple_of(at_ref[k] * XW, XW), XW) for k in range(NY)]
    copies = [
        pltpu.make_async_copy(w_ref.at[rows[k], :], w_vmem.at[k], sems.at[k]) for k in range(NY)
    ]
    for copy in copies:
        copy.start()
    square = sum(
        jnp.sum(jnp.square(q[...].astype(F32)), axis=1, keepdims=True) for q in blocks
    )
    scale = lax.rsqrt(square / (NY * XW) + EPS)
    acc_ref[...] = acts_ref[...].astype(F32)
    for k, q in enumerate(blocks):
        n = q[...].astype(F32) * scale * gain_ref[0:1, rows[k]]
        copies[k].wait()
        acc_ref[...] += jnp.dot(n.astype(BF), w_vmem[k], preferred_element_type=F32)
    out_ref[...] = acc_ref[...].astype(BF)


def run_out(at, blocks, gain, weight, acts):
    width = weight.shape[1]
    vmem = pl.BlockSpec(memory_space=pltpu.VMEM)
    blocks = [v.value if isinstance(v, Kept) else near(v) for v in blocks]
    return pl.pallas_call(
        out_kernel,
        in_specs=[pl.BlockSpec(memory_space=pltpu.SMEM)]
        + [vmem] * 6
        + [pl.BlockSpec(memory_space=pltpu.HBM)],
        out_specs=vmem,
        out_shape=shape_of(BF, ROWS, width),
        scratch_shapes=[
            pltpu.VMEM((ROWS, width), F32),
            pltpu.VMEM((NY, XW, width), BF),
            pltpu.SemaphoreType.DMA((NY,)),
        ],
        compiler_params=pltpu.CompilerParams(vmem_limit_bytes=28 << 20),
        name="gate_out",
    )(at, *blocks, gain, acts, far(weight))


def norm_kernel(at_ref, halo_ref, acts_ref, gain_ref, out_ref, full_ref):
    for start, ref in ((0, halo_ref), (HALO, acts_ref)):
        v = ref[...].astype(F32)
        scale = lax.rsqrt(jnp.mean(v * v, axis=1, keepdims=True) + EPS)
        full_ref[start : start + v.shape[0], :] = v * scale * gain_ref[0:1, :]
    for k in range(NX):
        start = pl.multiple_of(at_ref[k] * KX, KX)
        part = pltpu.roll(full_ref[:, pl.ds(start, KX)], at_ref[NX], 1)
        out_ref[:, k * KX : (k + 1) * KX] = part.astype(BF)


def run_norm(at, halo, acts, gain):
    width = acts.shape[1]
    return run(
        norm_kernel,
        (at,),
        (halo, acts, gain),
        [shape_of(BF, EXT, width)],
        [pltpu.VMEM((EXT, width), F32)],
        place=lambda v: v,
    )[0]


def columns_kernel(y_ref, shard_ref, o0, o1, o2, o3, all_ref):
    shard = shard_ref[...]
    for t in range(NY):
        x0, z0 = t * XW, 2304 + t * XW
        dt0, lv0 = 4352 + t * HEADS, 4384 + t * HEADS * 8
        all_ref[t, :, 0:XW] = shard[:, x0 : x0 + XW]
        all_ref[t, :, XW : XW + NS] = shard[:, 2048 : 2048 + NS]
        all_ref[t, :, XW + NS : WA] = jnp.concatenate(
            [
                shard[:, lv0 : lv0 + HEADS * 8].astype(F32),
                shard[:, dt0 : dt0 + HEADS].astype(F32),
                jnp.zeros((shard.shape[0], 128 - HEADS * 9), F32),
            ],
            axis=1,
        ).astype(BF)
        all_ref[t, :, WA : WA + XW] = shard[:, z0 : z0 + XW]
        all_ref[t, :, WA + XW :] = shard[:, 2048 + NS : 2304]
    for k, out in enumerate((o0, o1, o2, o3)):
        out[...] = all_ref[(y_ref[0] + k) % NY]


def run_columns(y, shard):
    rows = shard.shape[0]
    return run(
        columns_kernel,
        (y.reshape(1),),
        (shard,),
        [shape_of(BF, rows, WA + WB)] * 4,
        [pltpu.VMEM((NY, rows, WA + WB), BF)],
        place=lambda v: v,
    )


def join_kernel(y_ref, b0, b1, b2, b3, out_ref):
    rows = b0.shape[0]
    for back, block in ((0, b0), (3, b1), (2, b2), (1, b3)):
        start = pl.multiple_of(((y_ref[0] + back) % NY) * rows, rows)
        out_ref[pl.ds(start, rows), :] = block[...]


def run_join(y, blocks):
    rows, width = blocks[0].shape
    return run(join_kernel, (y.reshape(1),), blocks, [shape_of(BF, NY * rows, width)])[0]


def gather_kernel(*refs):
    *blocks, a_ref, b_ref = refs
    rows = blocks[0].shape[0]
    for k, block in enumerate(blocks):
        a_ref[k * rows : (k + 1) * rows, :] = block[:, :WA]
        b_ref[k * rows : (k + 1) * rows, :] = block[:, WA:]


def together(*values):
    return lax.optimization_barrier(values)


def ring_z(block):
    up, down = [block], [block]
    for k in range(4):
        up.append(sent(up[-1], Z_UP))
        if k < 3:
            down.append(sent(down[-1], Z_DOWN))
    return down + [up[4], up[3], up[2], up[1]]


def half_kernel(block_ref, out_ref, *, start):
    out_ref[...] = block_ref[start : start + out_ref.shape[0], :]


def rows_from(block, start, count):
    kernel = functools.partial(half_kernel, start=start)
    return run(kernel, (), (block,), [shape_of(BF, count, block.shape[1])])[0]


def near_pair(block, up, down):
    return sent(block, up), sent(block, down)


def far_pair(below, above, up, down, split):
    rest = above.shape[0] - split
    return sent(rows_from(below, 0, split), up), sent(rows_from(above, split, rest), down)


def mask_kernel(bits_ref, out_ref):
    for k in range(8):
        out_ref[k : k + 1, :] = jnp.full((1, XW), bits_ref[k], jnp.int32)


def layer(
    acts,
    in_proj,
    out_proj,
    conv_weight,
    conv_bias,
    dt_bias,
    decay_rate,
    skip_gain,
    level_bias,
    norm_gain,
    gate_gain,
):
    index = lax.axis_index("seq")
    y = index % NY
    z = (index // NY) % NZ
    x = index // (NY * NZ)
    w0, w1, w2, w3 = run_columns(y, in_proj[0])
    shared = (w0, sent(w1, Y_UP), sent(w2, Y_TWO), sent(w3, Y_DOWN))
    columns = run_join(y, shared)
    halo = sent(acts[0, ROWS - HALO :], HALO_NEXT)
    order = jnp.stack([x, (x + 3) % NX, (x + 1) % NX, (x + 2) % NX, (512 - 64 * z) % 512])
    u = run_norm(order, halo, acts[0], norm_gain)

    blocks = ring_z(columns)
    below, above = near_pair(u, Y_UP, Y_DOWN)
    far_lo, far_hi = far_pair(below, above, Y_UP, Y_DOWN, SPLIT)
    rows, rows_far = run(
        stack_kernel, (y.reshape(1),), (u, below, above, far_lo, far_hi),
        [plain(BF, NY, EXT, 3 * KX), plain(BF, NY, EXT, KX)],
    )
    depth = len(blocks) * blocks[1].shape[0]
    by_a, by_b = run(gather_kernel, (), blocks, [shape_of(BF, depth, WA), plain(BF, depth, WB)])

    y, zero, _ = together(y, jnp.zeros((), jnp.int32), blocks[7])
    piece = lambda v, width: lax.dynamic_slice_in_dim(v, y * width, width, v.ndim - 1)
    taps_a = jnp.concatenate(
        [piece(conv_weight[0, :, :2048], XW), conv_weight[0, :, 2048 : 2048 + NS]], axis=1
    )
    bias_a = jnp.concatenate(
        [piece(conv_bias[:, :2048], XW), conv_bias[:, 2048 : 2048 + NS]], axis=1
    )
    pad = jnp.zeros((1, 128 - HEADS * 9), F32)
    small_bias = jnp.concatenate(
        [piece(level_bias, HEADS * 8), piece(dt_bias, HEADS), pad], axis=1
    )
    rate = jnp.concatenate(
        [jnp.zeros((1, HEADS * 8), F32), piece(decay_rate, HEADS), pad], axis=1
    )
    skip = jnp.repeat(piece(skip_gain, HEADS), HD, axis=1)
    spreads = jnp.stack([spread(zero + k, 8) for k in range(8)] + [spread(zero + HEADS * 8, 1)])

    bits = jnp.stack([z & 1, (z >> 1) & 1, (z >> 2) & 1, x & 1, (x >> 1) & 1, zero, zero, zero])
    masks = run(mask_kernel, (bits,), (), [shape_of(jnp.int32, 8, XW)])[0]

    a_below, a_above = near_pair(by_a, X_UP, X_DOWN)
    fa_a, fb_a = far_pair(a_below, a_above, X_UP, X_DOWN, KX // 2)
    part_a = run_part(rows, by_a, a_below, a_above, shape_of)

    b_below, b_above = near_pair(by_b, X_UP, X_DOWN)
    w_far = sent(by_b, X_TWO)
    xs, b_mat, sp, cum, e2, sc, row, states, pair, logs, message = run_state(
        part_a, rows_far, fa_a, fb_a, taps_a, bias_a, small_bias, rate, spreads
    )
    part_b = run_part(rows, by_b, b_below, b_above, plain)

    gots = []
    for k, pairs in enumerate(EXCHANGES):
        got = sent(message, pairs)
        message, logs = run_merge(k, masks, got, message, logs)
        gots.append(got)

    y_part, c_mat, z_cols = run_intra(
        part_b, rows_far, w_far, conv_weight[0, :, 2048 + NS :], conv_bias[:, 2048 + NS :], skip,
        xs, b_mat, sp, cum, e2, row, states, pair, spreads,
    )
    block = lambda k: (y + k) % NY
    order = jnp.stack([block(k) for k in range(NY)])
    q0, q1, q2, q3 = run_cross(order, y_part, c_mat, sc, z_cols, gots, logs, spreads)
    back_two = sent(q2, Y_TWO)
    blocks = (q0, sent(q1, Y_UP), back_two, sent(q3, Y_DOWN))
    heads_at = jnp.stack([block(0), block(3), block(2), block(1)])
    result = run_out(heads_at, blocks, gate_gain, out_proj[0], acts[0])
    return lax.ppermute(result, "section", [(0, 1), (1, 0)])[None]


def solution(mesh):
    return jax.shard_map(
        layer,
        mesh=mesh,
        in_specs=(
            P("section", "seq", None),
            P("section", "seq", None),
            P("section", None, None),
            P("section", None, None),
            P("section", None),
            P("section", None),
            P("section", None),
            P("section", None),
            P("section", None),
            P("section", None),
            P("section", None),
        ),
        out_specs=P("section", "seq", None),
        check_vma=False,
    )
```

```python
import functools

import jax
import jax.numpy as jnp
from jax import lax
from jax.experimental import pallas as pl
from jax.experimental.pallas import tpu as pltpu
from jax.sharding import PartitionSpec as P

EPS = 1e-05
F32 = jnp.float32
BF = jnp.bfloat16


NX, NZ, NY = 4, 8, 4
ROWS = 256
HEADS = 8
HD = 64
XW = HEADS * HD
NS = 128
HALO = 16
WA, WB = 768, 640
EXT = ROWS + HALO
SPLIT = 144
KX = 512


def route(move):
    pairs = []
    for x in range(NX):
        for z in range(NZ):
            for y in range(NY):
                a, b, c = move(x, z, y)
                pairs.append(
                    ((x * NZ + z) * NY + y, ((a % NX) * NZ + b % NZ) * NY + c % NY)
                )
    return pairs


X_UP = route(lambda x, z, y: (x + 1, z, y))
X_DOWN = route(lambda x, z, y: (x - 1, z, y))
X_TWO = route(lambda x, z, y: (x + 2, z, y))
Z_UP = route(lambda x, z, y: (x, z + 1, y))
Z_DOWN = route(lambda x, z, y: (x, z - 1, y))
Y_UP = route(lambda x, z, y: (x, z, y + 1))
Y_DOWN = route(lambda x, z, y: (x, z, y - 1))
Y_TWO = route(lambda x, z, y: (x, z, y + 2))
HALO_NEXT = [(i, i + 1) for i in range(NX * NZ * NY - 1)]
EXCHANGES = [
    route(lambda x, z, y: (x, z ^ 1, y)),
    route(lambda x, z, y: (x, z ^ 2, y)),
    route(lambda x, z, y: (x, 7 - z, y)),
    route(lambda x, z, y: (x ^ 1, z, y)),
    route(lambda x, z, y: (3 - x, z, y)),
]


def sent(value, pairs):
    return lax.ppermute(getattr(value, "value", value), "seq", pairs)


def spread_kernel(out_ref):
    row = lax.broadcasted_iota(jnp.int32, (128, XW), 0)
    head = lax.broadcasted_iota(jnp.int32, (128, XW), 1) // HD
    for k in range(9):
        lane = HEADS * 8 + head if k == 8 else k + 8 * head
        out_ref[k] = jnp.where(row == lane, 1.0, 0.0).astype(BF)


def mm(a, b):
    return jnp.dot(a.astype(BF), b.astype(BF), preferred_element_type=F32)


def softplus(v):
    return jnp.maximum(v, 0.0) + jnp.log1p(jnp.exp(-jnp.abs(v)))


def silu(v):
    half = 0.5 * v
    return half + half * jnp.tanh(half)


def conv_block(wide, taps, bias):
    mixed = bias[0:1, :] + taps[0:1, :] * wide[HALO - 3 : HALO - 3 + ROWS, :]
    for k in range(1, 4):
        mixed = mixed + taps[k : k + 1, :] * wide[HALO - 3 + k : HALO - 3 + k + ROWS, :]
    return silu(mixed)


def shape_of(dtype, *shape):
    return pltpu.VMEM(shape, dtype)


class Kept:
    def __init__(self, value, out):
        self.value = self.loose = value
        if out.memory_space == pltpu.HBM:
            self.value = far(value)
        self.shape = value.shape
        self.dtype = value.dtype


def plain(dtype, *shape):
    return pltpu.HBM(shape, dtype)


def near(value):
    return pltpu.with_memory_space_constraint(value, pltpu.VMEM)


def far(value):
    return pltpu.with_memory_space_constraint(value, pltpu.HBM)


def run(kernel, scalars, arrays, outs, scratch=(), place=near, loose=False):
    smem = pl.BlockSpec(memory_space=pltpu.SMEM)
    vmem = pl.BlockSpec(memory_space=pltpu.VMEM)
    kept = lambda v: v.loose if loose else v.value
    arrays = [kept(v) if isinstance(v, Kept) else place(v) for v in arrays]
    results = pl.pallas_call(
        kernel,
        in_specs=[smem] * len(scalars) + [vmem] * len(arrays),
        out_specs=[vmem] * len(outs),
        out_shape=outs,
        scratch_shapes=list(scratch),
        compiler_params=pltpu.CompilerParams(vmem_limit_bytes=10 << 20),
    )(*scalars, *arrays)
    return [Kept(v, out) for v, out in zip(results, outs, strict=True)]


def each_block(body):
    def step(j, carry):
        body(j)
        return carry

    lax.fori_loop(0, NY, step, 0)


def part_kernel(rows_ref, own_ref, below_ref, above_ref, out_ref):
    def block(j):
        total = None
        for k, w_ref in enumerate((own_ref, below_ref, above_ref)):
            there = rows_ref[j, :, k * KX : (k + 1) * KX]
            part = jnp.dot(there, w_ref[...], preferred_element_type=F32)
            total = part if total is None else total + part
        out_ref[j] = total

    each_block(block)


def run_part(rows, own, below, above, where):
    out = where(F32, NY, EXT, own.shape[1])
    return run(part_kernel, (), (rows, own, below, above), [out])[0]


def stack_kernel(y_ref, own_ref, below_ref, above_ref, lo_ref, hi_ref, near_ref, far_ref):
    y = y_ref[0]
    edge = 3 * KX
    for out_ref, a, b in ((near_ref, 0, edge), (far_ref, edge, edge + KX)):
        out_ref[y] = own_ref[:, a:b]
        out_ref[(y + 3) % NY] = below_ref[:, a:b]
        out_ref[(y + 1) % NY] = above_ref[:, a:b]
        out_ref[(y + 2) % NY, 0:SPLIT, :] = lo_ref[:, a:b]
        out_ref[(y + 2) % NY, SPLIT:, :] = hi_ref[:, a:b]


def finished(part_ref, rows_ref, fa_ref, fb_ref, j):
    total = (
        part_ref[j]
        + jnp.dot(rows_ref[j, :, : KX // 2], fa_ref[...], preferred_element_type=F32)
        + jnp.dot(rows_ref[j, :, KX // 2 :], fb_ref[...], preferred_element_type=F32)
    )
    return total.astype(BF).astype(F32)


def state_kernel(
    part_ref, rows_ref, fa_ref, fb_ref, taps_ref, bias_ref, small_bias_ref, rate_ref, spread_ref,
    xs_ref, b_ref, sp_ref, cum_ref, e2_ref, sc_ref, row_ref, s_ref, pair_ref, logs_ref, msg_ref,
    wide_ref, acc_ref, carry_ref,
):
    acc_ref[...] = jnp.zeros_like(acc_ref)
    carry_ref[...] = jnp.zeros_like(carry_ref)
    logs_ref[...] = jnp.zeros_like(logs_ref)

    def block(j):
        p = finished(part_ref, rows_ref, fa_ref, fb_ref, j)
        wide_ref[...] = p[:, : XW + NS]
        mixed = conv_block(wide_ref, taps_ref, bias_ref)
        xs = mixed[:, :XW]
        b_mat = mixed[:, XW:]
        sp = softplus(p[HALO:, XW + NS :] + small_bias_ref[0:1, :])
        g = -sp * rate_ref[0:1, :]
        row = lax.broadcasted_iota(jnp.int32, (ROWS, ROWS), 0)
        col = lax.broadcasted_iota(jnp.int32, (ROWS, ROWS), 1)
        tri = jnp.where(col <= row, 1.0, 0.0).astype(BF)
        g0 = g.astype(BF)
        r1 = g - g0.astype(F32)
        g1 = r1.astype(BF)
        g2 = r1 - g1.astype(F32)
        cum = mm(tri, g0) + mm(tri, g1) + mm(tri, g2)
        last = cum[ROWS - 1 : ROWS, :]
        tail = jnp.exp(last - cum) * sp
        head_spread = spread_ref[8]
        xt = xs * mm(tail, head_spread)
        state = mm(b_mat.T, xt)
        last8 = jnp.broadcast_to(last, (16, 128))
        hi = last8.astype(BF)
        rest = last8 - hi.astype(F32)
        mid = rest.astype(BF)
        low = rest - mid.astype(F32)
        last_wide = mm(hi, head_spread) + mm(mid, head_spread) + mm(low, head_spread)
        acc = jnp.exp(last_wide[0:1, :]) * acc_ref[...] + state
        acc_ref[...] = acc
        group = carry_ref[0:1, :]
        pair = jnp.where(j == 2, 0.0, carry_ref[1:2, :])
        e2_ref[j] = jnp.exp(cum + pair)
        lane = lax.broadcasted_iota(jnp.int32, (128, 128), 1)
        src = lax.broadcasted_iota(jnp.int32, (128, 128), 0)
        to_levels = jnp.where(src - HEADS * 8 == lane // 8, 1.0, 0.0)
        sc_ref[j] = (sp * mm(jnp.exp(cum + group), to_levels)).astype(BF)
        carry_ref[0:1, :] = group + last
        carry_ref[1:2, :] = pair + last
        xs_ref[j] = xs
        b_ref[j] = b_mat.astype(BF)
        sp_ref[j] = sp
        cum_ref[j] = cum
        row_ref[j] = cum.T[HEADS * 8 : HEADS * 9, :]
        s_ref[j] = state.astype(BF)
        logs_ref[0:1, :] = logs_ref[0:1, :] + last_wide[0:1, :]

        @pl.when(j == 1)
        def _():
            pair_ref[...] = acc.astype(BF)

        @pl.when(j == NY - 1)
        def _():
            pack_message(msg_ref, acc, logs_ref[0:1, :])

    each_block(block)


def pack_message(msg_ref, state, log):
    msg_ref[0:NS, :] = state.astype(BF)
    hi = log.astype(BF).astype(F32)
    row = lax.broadcasted_iota(jnp.int32, (16, XW), 0)
    both = jnp.where(row == 0, hi, jnp.where(row == 1, log - hi, 0.0))
    msg_ref[NS:, :] = both.astype(BF)


def run_state(part, rows, far_a, far_b, taps, bias, small_bias, rate, spreads):
    return run(
        state_kernel,
        (),
        (part, rows, far_a, far_b, taps, bias, small_bias, rate, spreads),
        [
            plain(F32, NY, ROWS, XW), plain(BF, NY, ROWS, NS), plain(F32, NY, ROWS, 128),
            plain(F32, NY, ROWS, 128), plain(F32, NY, ROWS, 128), plain(BF, NY, ROWS, 128),
            plain(F32, NY, HEADS, ROWS), plain(BF, NY, NS, XW),
            plain(BF, NS, XW), shape_of(F32, 16, XW), shape_of(BF, NS + 16, XW),
        ],
        [
            pltpu.VMEM((EXT, XW + NS), F32),
            pltpu.VMEM((NS, XW), F32),
            pltpu.VMEM((8, 128), F32),
        ],
    )


def intra_kernel(
    part_ref, rows_ref, far_ref, taps_ref, bias_ref, skip_ref,
    xs_ref, b_ref, sp_ref, cum_ref, e2_ref, row_ref, s1_ref, s2_ref, spread_ref,
    y_ref, c_ref, z_ref, wide_ref, *, base,
):
    j = pl.program_id(0) + base
    p = part_ref[0] + jnp.dot(rows_ref[0], far_ref[...], preferred_element_type=F32)
    p = p.astype(BF).astype(F32)
    z_ref[0] = p[HALO:, :XW].astype(BF)
    wide_ref[...] = p[:, XW:]
    c_mat = conv_block(wide_ref, taps_ref, bias_ref).astype(BF)
    c_ref[0] = c_mat
    xs = xs_ref[0]
    sp = sp_ref[0].astype(BF)
    cum = cum_ref[0]
    scores = lax.dot_general(
        c_mat, b_ref[0], (((1,), (1,)), ((), ())), preferred_element_type=F32
    )
    row = lax.broadcasted_iota(jnp.int32, (ROWS, ROWS), 0)
    col = lax.broadcasted_iota(jnp.int32, (ROWS, ROWS), 1)
    causal = col <= row
    head_spread = spread_ref[8]
    xd = (xs * mm(sp, head_spread)).astype(BF)
    parts = []
    for h in range(HEADS):
        lane = HEADS * 8 + h
        diff = cum[:, lane : lane + 1] - row_ref[0, h : h + 1, :]
        decay = jnp.exp(jnp.where(causal, diff, -1e30)) * scores
        parts.append(mm(decay, xd[:, h * HD : (h + 1) * HD]))
    y = jnp.concatenate(parts, axis=1) * mm(sp, spread_ref[0])
    y = y + skip_ref[0:1, :] * xs
    odd = (j % 2).astype(F32)
    late = (j // 2).astype(F32)
    one = mm(sp, spread_ref[1]) * mm(jnp.exp(cum), head_spread)
    y = y + mm(c_mat, s1_ref[0]) * (one * odd)
    two = mm(sp, spread_ref[2]) * mm(e2_ref[0], head_spread)
    y = y + mm(c_mat, s2_ref[...]) * (two * late)
    y_ref[0] = y


def run_intra(base, part, rows, w_far, taps, bias, skip, xs, b_mat, sp, cum, e2, row, states, pair, spreads):
    whole = lambda *shape: pl.BlockSpec(shape, lambda j: (0,) * len(shape))
    each = lambda a, b: pl.BlockSpec((1, a, b), lambda j: (j + base, 0, 0))
    own = lambda a, b: pl.BlockSpec((1, a, b), lambda j: (j, 0, 0))
    arrays = (part, rows, w_far, taps, bias, skip, xs, b_mat, sp, cum, e2, row, states, pair, spreads)
    arrays = [v.value if isinstance(v, Kept) else far(v) for v in arrays]
    half = NY // 2
    outs = [plain(F32, half, ROWS, XW), plain(BF, half, ROWS, NS), plain(BF, half, ROWS, XW)]
    results = pl.pallas_call(
        functools.partial(intra_kernel, base=base),
        grid=(half,),
        in_specs=[
            each(EXT, WB), each(EXT, KX), whole(KX, WB),
            whole(4, NS), whole(1, NS), whole(1, XW),
            each(ROWS, XW), each(ROWS, NS), each(ROWS, 128), each(ROWS, 128), each(ROWS, 128),
            each(HEADS, ROWS),
            pl.BlockSpec((1, NS, XW), lambda j: (base, 0, 0)),
            whole(NS, XW), whole(9, 128, XW),
        ],
        out_specs=[own(ROWS, XW), own(ROWS, NS), own(ROWS, XW)],
        out_shape=outs,
        scratch_shapes=[pltpu.VMEM((EXT, NS), F32)],
        compiler_params=pltpu.CompilerParams(vmem_limit_bytes=28 << 20),
        name="intra_block",
    )(*arrays)
    return [Kept(v, out) for v, out in zip(results, outs, strict=True)]


def merge_kernel(mask_ref, got_ref, own_ref, logs_ref, msg_ref, new_logs_ref, *, k):
    upper = mask_ref[k : k + 1, :] == 1
    other = got_ref[0:NS, :].astype(F32)
    tail = got_ref[NS:, :].astype(F32)
    other_log = tail[0:1, :] + tail[1:2, :]
    log = logs_ref[0:1, :]
    before = logs_ref[1:2, :]
    state = (
        jnp.where(upper, jnp.exp(log), 1.0) * other
        + jnp.where(upper, 1.0, jnp.exp(other_log)) * own_ref[0:NS, :].astype(F32)
    )
    log = log + other_log
    new_logs_ref[...] = logs_ref[...]
    new_logs_ref[0:1, :] = log
    new_logs_ref[1:2, :] = jnp.where(upper, before + other_log, before)
    new_logs_ref[8 + k : 9 + k, :] = jnp.where(upper, jnp.exp(before), 0.0)
    pack_message(msg_ref, state, log)


def run_merge(k, masks, got, own, logs):
    return run(
        functools.partial(merge_kernel, k=k),
        (),
        (masks, got, own, logs),
        [shape_of(BF, NS + 16, XW), shape_of(F32, 16, XW)],
    )


def cross_kernel(
    at_ref, ya_ref, ca_ref, za_ref, yb_ref, cb_ref, zb_ref, sc_ref, g3, g4, g5, g6, g7, logs_ref, spread_ref,
    q0, q1, q2, q3, bucket_ref,
):
    for k, got in enumerate((g3, g4, g5, g6, g7)):
        scaled = got[0:NS, :].astype(F32) * logs_ref[8 + k : 9 + k, :]
        bucket_ref[k] = scaled.astype(BF)
    for k, q_ref in enumerate((q0, q1, q2, q3)):
        j = (at_ref[0] + k) % NY
        first = j < NY // 2
        near_j = j % (NY // 2)
        c_mat = jnp.where(first, ca_ref[near_j], cb_ref[near_j])
        scale = sc_ref[j]
        y = jnp.where(first, ya_ref[near_j], yb_ref[near_j])
        gate = jnp.where(first, za_ref[near_j], zb_ref[near_j]).astype(F32)
        for level in range(3, 8):
            y = y + mm(c_mat, bucket_ref[level - 3]) * mm(scale, spread_ref[level])
        q_ref[...] = (y * silu(gate)).astype(BF)


def run_cross(at, inner, sc, gots, logs, spreads):
    return run(
        cross_kernel,
        (at,),
        (*inner, sc, *gots, logs, spreads),
        [shape_of(BF, ROWS, XW)] * NY,
        [pltpu.VMEM((5, NS, XW), BF)],
        place=lambda v: v,
    )


def out_kernel(at_ref, q0, q1, q2, q3, gain_ref, acts_ref, w_ref, out_ref, acc_ref, w_vmem, sems):
    blocks = (q0, q1, q2, q3)
    rows = [
        pl.ds(pl.multiple_of(((at_ref[0] + NY - k) % NY) * XW, XW), XW) for k in range(NY)
    ]
    copies = [
        pltpu.make_async_copy(w_ref.at[rows[k], :], w_vmem.at[k], sems.at[k]) for k in range(NY)
    ]
    for copy in copies:
        copy.start()
    square = sum(
        jnp.sum(jnp.square(q[...].astype(F32)), axis=1, keepdims=True) for q in blocks
    )
    scale = lax.rsqrt(square / (NY * XW) + EPS)
    acc_ref[...] = acts_ref[...].astype(F32)
    for k, q in enumerate(blocks):
        n = q[...].astype(F32) * scale * gain_ref[0:1, rows[k]]
        copies[k].wait()
        acc_ref[...] += jnp.dot(n.astype(BF), w_vmem[k], preferred_element_type=F32)
    out_ref[...] = acc_ref[...].astype(BF)


def run_out(at, blocks, gain, weight, acts):
    width = weight.shape[1]
    vmem = pl.BlockSpec(memory_space=pltpu.VMEM)
    blocks = [v.value if isinstance(v, Kept) else near(v) for v in blocks]
    return pl.pallas_call(
        out_kernel,
        in_specs=[pl.BlockSpec(memory_space=pltpu.SMEM)]
        + [vmem] * 6
        + [pl.BlockSpec(memory_space=pltpu.HBM)],
        out_specs=vmem,
        out_shape=shape_of(BF, ROWS, width),
        scratch_shapes=[
            pltpu.VMEM((ROWS, width), F32),
            pltpu.VMEM((NY, XW, width), BF),
            pltpu.SemaphoreType.DMA((NY,)),
        ],
        compiler_params=pltpu.CompilerParams(vmem_limit_bytes=28 << 20),
        name="gate_out",
    )(at, *blocks, gain, acts, far(weight))


def norm_kernel(at_ref, halo_ref, acts_ref, gain_ref, out_ref, full_ref):
    for start, ref in ((0, halo_ref), (HALO, acts_ref)):
        v = ref[...].astype(F32)
        scale = lax.rsqrt(jnp.mean(v * v, axis=1, keepdims=True) + EPS)
        full_ref[start : start + v.shape[0], :] = v * scale * gain_ref[0:1, :]
    for k in range(NX):
        start = pl.multiple_of(at_ref[1 + k] * KX, KX)
        part = pltpu.roll(full_ref[:, pl.ds(start, KX)], at_ref[1 + NX], 1)
        out_ref[:, k * KX : (k + 1) * KX] = part.astype(BF)


def run_norm(at, halo, acts, gain):
    width = acts.shape[1]
    return run(
        norm_kernel,
        (at,),
        (halo, acts, gain),
        [shape_of(BF, EXT, width)],
        [pltpu.VMEM((EXT, width), F32)],
        place=lambda v: v,
    )[0]


def columns_kernel(y_ref, shard_ref, o0, o1, o2, o3, all_ref):
    shard = shard_ref[...]
    for t in range(NY):
        x0, z0 = t * XW, 2304 + t * XW
        dt0, lv0 = 4352 + t * HEADS, 4384 + t * HEADS * 8
        all_ref[t, :, 0:XW] = shard[:, x0 : x0 + XW]
        all_ref[t, :, XW : XW + NS] = shard[:, 2048 : 2048 + NS]
        all_ref[t, :, XW + NS : WA] = jnp.concatenate(
            [
                shard[:, lv0 : lv0 + HEADS * 8].astype(F32),
                shard[:, dt0 : dt0 + HEADS].astype(F32),
                jnp.zeros((shard.shape[0], 128 - HEADS * 9), F32),
            ],
            axis=1,
        ).astype(BF)
        all_ref[t, :, WA : WA + XW] = shard[:, z0 : z0 + XW]
        all_ref[t, :, WA + XW :] = shard[:, 2048 + NS : 2304]
    for k, out in enumerate((o0, o1, o2, o3)):
        out[...] = all_ref[(y_ref[0] + k) % NY]


def run_columns(y, shard):
    rows = shard.shape[0]
    return run(
        columns_kernel,
        (y,),
        (shard,),
        [shape_of(BF, rows, WA + WB)] * 4,
        [pltpu.VMEM((NY, rows, WA + WB), BF)],
        place=lambda v: v,
    )


def join_kernel(y_ref, b0, b1, b2, b3, out_ref):
    rows = b0.shape[0]
    for back, block in ((0, b0), (3, b1), (2, b2), (1, b3)):
        start = pl.multiple_of(((y_ref[0] + back) % NY) * rows, rows)
        out_ref[pl.ds(start, rows), :] = block[...]


def run_join(y, blocks):
    rows, width = blocks[0].shape
    return run(join_kernel, (y,), blocks, [shape_of(BF, NY * rows, width)])[0]


def gather_kernel(*refs):
    *blocks, a_ref, b_ref = refs
    rows = blocks[0].shape[0]
    for k, block in enumerate(blocks):
        a_ref[k * rows : (k + 1) * rows, :] = block[:, :WA]
        b_ref[k * rows : (k + 1) * rows, :] = block[:, WA:]


def together(*values):
    return lax.optimization_barrier(values)


def ring_z(block):
    up, down = [block], [block]
    for k in range(4):
        up.append(sent(up[-1], Z_UP))
        if k < 3:
            down.append(sent(down[-1], Z_DOWN))
    return down + [up[4], up[3], up[2], up[1]]


def half_kernel(block_ref, out_ref, *, start):
    out_ref[...] = block_ref[start : start + out_ref.shape[0], :]


def rows_from(block, start, count):
    kernel = functools.partial(half_kernel, start=start)
    return run(kernel, (), (block,), [shape_of(BF, count, block.shape[1])])[0]


def near_pair(block, up, down):
    return sent(block, up), sent(block, down)


def far_pair(below, above, up, down, split):
    rest = above.shape[0] - split
    return sent(rows_from(below, 0, split), up), sent(rows_from(above, split, rest), down)


def mask_kernel(bits_ref, out_ref):
    for k in range(5):
        out_ref[k : k + 1, :] = jnp.full((1, XW), bits_ref[2 + NX + k], jnp.int32)


def layer(
    acts,
    in_proj,
    out_proj,
    conv_weight,
    conv_bias,
    dt_bias,
    decay_rate,
    skip_gain,
    level_bias,
    norm_gain,
    gate_gain,
):
    index = lax.axis_index("seq")
    y = index % NY
    z = (index // NY) % NZ
    x = index // (NY * NZ)
    bits = [z & 1, (z >> 1) & 1, (z >> 2) & 1, x & 1, (x >> 1) & 1]
    where = jnp.stack(
        [y, x, (x + 3) % NX, (x + 1) % NX, (x + 2) % NX, (512 - 64 * z) % 512, *bits]
    )
    w0, w1, w2, w3 = run_columns(where, in_proj[0])
    shared = (w0, sent(w1, Y_UP), sent(w2, Y_TWO), sent(w3, Y_DOWN))
    columns = run_join(where, shared)
    halo = sent(acts[0, ROWS - HALO :], HALO_NEXT)
    u = run_norm(where, halo, acts[0], norm_gain)

    blocks = ring_z(columns)
    below, above = near_pair(u, Y_UP, Y_DOWN)
    far_lo, far_hi = far_pair(below, above, Y_UP, Y_DOWN, SPLIT)
    rows, rows_far = run(
        stack_kernel, (where,), (u, below, above, far_lo, far_hi),
        [plain(BF, NY, EXT, 3 * KX), plain(BF, NY, EXT, KX)],
    )
    depth = len(blocks) * blocks[1].shape[0]
    by_a, by_b = run(gather_kernel, (), blocks, [shape_of(BF, depth, WA), plain(BF, depth, WB)])

    y, _ = together(y, blocks[7])
    piece = lambda v, width: lax.dynamic_slice_in_dim(v, y * width, width, v.ndim - 1)
    taps_a = jnp.concatenate(
        [piece(conv_weight[0, :, :2048], XW), conv_weight[0, :, 2048 : 2048 + NS]], axis=1
    )
    bias_a = jnp.concatenate(
        [piece(conv_bias[:, :2048], XW), conv_bias[:, 2048 : 2048 + NS]], axis=1
    )
    pad = jnp.zeros((1, 128 - HEADS * 9), F32)
    small_bias = jnp.concatenate(
        [piece(level_bias, HEADS * 8), piece(dt_bias, HEADS), pad], axis=1
    )
    rate = jnp.concatenate(
        [jnp.zeros((1, HEADS * 8), F32), piece(decay_rate, HEADS), pad], axis=1
    )
    skip = jnp.repeat(piece(skip_gain, HEADS), HD, axis=1)
    spreads = run(spread_kernel, (), (), [plain(BF, 9, 128, XW)])[0]
    masks = run(mask_kernel, (where,), (), [shape_of(jnp.int32, 8, XW)])[0]

    a_below, a_above = near_pair(by_a, X_UP, X_DOWN)
    fa_a, fb_a = far_pair(a_below, a_above, X_UP, X_DOWN, KX // 2)
    part_a = run_part(rows, by_a, a_below, a_above, shape_of)

    b_below, b_above = near_pair(by_b, X_UP, X_DOWN)
    w_far = sent(by_b, X_TWO)
    xs, b_mat, sp, cum, e2, sc, row, states, pair, logs, message = run_state(
        part_a, rows_far, fa_a, fb_a, taps_a, bias_a, small_bias, rate, spreads
    )
    part_b = run_part(rows, by_b, b_below, b_above, plain)

    gots = []
    for k, pairs in enumerate(EXCHANGES):
        got = sent(message, pairs)
        message, logs = run_merge(k, masks, got, message, logs)
        gots.append(got)

    inner = []
    for base in (0, NY // 2):
        inner += run_intra(
            base, part_b, rows_far, w_far, conv_weight[0, :, 2048 + NS :], conv_bias[:, 2048 + NS :], skip,
            xs, b_mat, sp, cum, e2, row, states, pair, spreads,
        )
    q0, q1, q2, q3 = run_cross(where, inner, sc, gots, logs, spreads)
    back_two = sent(q2, Y_TWO)
    blocks = (q0, sent(q1, Y_UP), back_two, sent(q3, Y_DOWN))
    result = run_out(where, blocks, gate_gain, out_proj[0], acts[0])
    return lax.ppermute(result, "section", [(0, 1), (1, 0)])[None]


def solution(mesh):
    return jax.shard_map(
        layer,
        mesh=mesh,
        in_specs=(
            P("section", "seq", None),
            P("section", "seq", None),
            P("section", None, None),
            P("section", None, None),
            P("section", None),
            P("section", None),
            P("section", None),
            P("section", None),
            P("section", None),
            P("section", None),
            P("section", None),
        ),
        out_specs=P("section", "seq", None),
        check_vma=False,
    )
```

```python
import functools

import jax
import jax.numpy as jnp
from jax import lax
from jax.experimental import pallas as pl
from jax.experimental.pallas import tpu as pltpu
from jax.sharding import PartitionSpec as P

EPS = 1e-05
F32 = jnp.float32
BF = jnp.bfloat16


NX, NZ, NY = 4, 8, 4
ROWS = 256
HEADS = 8
HD = 64
XW = HEADS * HD
NS = 128
HALO = 16
WA, WB = 768, 640
EXT = ROWS + HALO
SPLIT = 144
KX = 512


def route(move):
    pairs = []
    for x in range(NX):
        for z in range(NZ):
            for y in range(NY):
                a, b, c = move(x, z, y)
                pairs.append(
                    ((x * NZ + z) * NY + y, ((a % NX) * NZ + b % NZ) * NY + c % NY)
                )
    return pairs


X_UP = route(lambda x, z, y: (x + 1, z, y))
X_DOWN = route(lambda x, z, y: (x - 1, z, y))
X_TWO = route(lambda x, z, y: (x + 2, z, y))
Z_UP = route(lambda x, z, y: (x, z + 1, y))
Z_DOWN = route(lambda x, z, y: (x, z - 1, y))
Y_UP = route(lambda x, z, y: (x, z, y + 1))
Y_DOWN = route(lambda x, z, y: (x, z, y - 1))
Y_TWO = route(lambda x, z, y: (x, z, y + 2))
HALO_NEXT = [(i, i + 1) for i in range(NX * NZ * NY - 1)]
EXCHANGES = [
    route(lambda x, z, y: (x, z ^ 1, y)),
    route(lambda x, z, y: (x, z ^ 2, y)),
    route(lambda x, z, y: (x, 7 - z, y)),
    route(lambda x, z, y: (x ^ 1, z, y)),
    route(lambda x, z, y: (3 - x, z, y)),
]


def sent(value, pairs):
    return lax.ppermute(getattr(value, "value", value), "seq", pairs)


def spread_kernel(out_ref):
    row = lax.broadcasted_iota(jnp.int32, (128, XW), 0)
    head = lax.broadcasted_iota(jnp.int32, (128, XW), 1) // HD
    for k in range(9):
        lane = HEADS * 8 + head if k == 8 else k + 8 * head
        out_ref[k] = jnp.where(row == lane, 1.0, 0.0).astype(BF)


def mm(a, b):
    return jnp.dot(a.astype(BF), b.astype(BF), preferred_element_type=F32)


def softplus(v):
    return jnp.maximum(v, 0.0) + jnp.log1p(jnp.exp(-jnp.abs(v)))


def silu(v):
    half = 0.5 * v
    return half + half * jnp.tanh(half)


def conv_block(wide, taps, bias):
    mixed = bias[0:1, :] + taps[0:1, :] * wide[HALO - 3 : HALO - 3 + ROWS, :]
    for k in range(1, 4):
        mixed = mixed + taps[k : k + 1, :] * wide[HALO - 3 + k : HALO - 3 + k + ROWS, :]
    return silu(mixed)


def shape_of(dtype, *shape):
    return pltpu.VMEM(shape, dtype)


class Kept:
    def __init__(self, value, out):
        self.value = self.loose = value
        if out.memory_space == pltpu.HBM:
            self.value = far(value)
        self.shape = value.shape
        self.dtype = value.dtype


def plain(dtype, *shape):
    return pltpu.HBM(shape, dtype)


def near(value):
    return pltpu.with_memory_space_constraint(value, pltpu.VMEM)


def far(value):
    return pltpu.with_memory_space_constraint(value, pltpu.HBM)


def run(kernel, scalars, arrays, outs, scratch=(), place=near, loose=False):
    smem = pl.BlockSpec(memory_space=pltpu.SMEM)
    vmem = pl.BlockSpec(memory_space=pltpu.VMEM)
    kept = lambda v: v.loose if loose else v.value
    arrays = [kept(v) if isinstance(v, Kept) else place(v) for v in arrays]
    results = pl.pallas_call(
        kernel,
        in_specs=[smem] * len(scalars) + [vmem] * len(arrays),
        out_specs=[vmem] * len(outs),
        out_shape=outs,
        scratch_shapes=list(scratch),
        compiler_params=pltpu.CompilerParams(vmem_limit_bytes=10 << 20),
    )(*scalars, *arrays)
    return [Kept(v, out) for v, out in zip(results, outs, strict=True)]


def each_block(body):
    def step(j, carry):
        body(j)
        return carry

    lax.fori_loop(0, NY, step, 0)


def part_kernel(rows_ref, own_ref, below_ref, above_ref, out_ref):
    def block(j):
        total = None
        for k, w_ref in enumerate((own_ref, below_ref, above_ref)):
            there = rows_ref[j, :, k * KX : (k + 1) * KX]
            part = jnp.dot(there, w_ref[...], preferred_element_type=F32)
            total = part if total is None else total + part
        out_ref[j] = total

    each_block(block)


def run_part(rows, own, below, above, where):
    out = where(F32, NY, EXT, own.shape[1])
    return run(part_kernel, (), (rows, own, below, above), [out])[0]


def stack_kernel(y_ref, own_ref, below_ref, above_ref, lo_ref, hi_ref, near_ref, far_ref):
    y = y_ref[0]
    edge = 3 * KX
    for out_ref, a, b in ((near_ref, 0, edge), (far_ref, edge, edge + KX)):
        out_ref[y] = own_ref[:, a:b]
        out_ref[(y + 3) % NY] = below_ref[:, a:b]
        out_ref[(y + 1) % NY] = above_ref[:, a:b]
        out_ref[(y + 2) % NY, 0:SPLIT, :] = lo_ref[:, a:b]
        out_ref[(y + 2) % NY, SPLIT:, :] = hi_ref[:, a:b]


def finished(part_ref, rows_ref, fa_ref, fb_ref, j):
    total = (
        part_ref[j]
        + jnp.dot(rows_ref[j, :, : KX // 2], fa_ref[...], preferred_element_type=F32)
        + jnp.dot(rows_ref[j, :, KX // 2 :], fb_ref[...], preferred_element_type=F32)
    )
    return total.astype(BF).astype(F32)


def state_kernel(
    part_ref, rows_ref, fa_ref, fb_ref, taps_ref, bias_ref, small_bias_ref, rate_ref, spread_ref,
    xs_ref, b_ref, sp_ref, cum_ref, e2_ref, sc_ref, row_ref, s_ref, pair_ref, logs_ref, msg_ref,
    wide_ref, acc_ref, carry_ref,
):
    acc_ref[...] = jnp.zeros_like(acc_ref)
    carry_ref[...] = jnp.zeros_like(carry_ref)
    logs_ref[...] = jnp.zeros_like(logs_ref)

    def block(j):
        p = finished(part_ref, rows_ref, fa_ref, fb_ref, j)
        wide_ref[...] = p[:, : XW + NS]
        mixed = conv_block(wide_ref, taps_ref, bias_ref)
        xs = mixed[:, :XW]
        b_mat = mixed[:, XW:]
        sp = softplus(p[HALO:, XW + NS :] + small_bias_ref[0:1, :])
        g = -sp * rate_ref[0:1, :]
        row = lax.broadcasted_iota(jnp.int32, (ROWS, ROWS), 0)
        col = lax.broadcasted_iota(jnp.int32, (ROWS, ROWS), 1)
        tri = jnp.where(col <= row, 1.0, 0.0).astype(BF)
        g0 = g.astype(BF)
        r1 = g - g0.astype(F32)
        g1 = r1.astype(BF)
        g2 = r1 - g1.astype(F32)
        cum = mm(tri, g0) + mm(tri, g1) + mm(tri, g2)
        last = cum[ROWS - 1 : ROWS, :]
        tail = jnp.exp(last - cum) * sp
        head_spread = spread_ref[8]
        xt = xs * mm(tail, head_spread)
        state = mm(b_mat.T, xt)
        last8 = jnp.broadcast_to(last, (16, 128))
        hi = last8.astype(BF)
        rest = last8 - hi.astype(F32)
        mid = rest.astype(BF)
        low = rest - mid.astype(F32)
        last_wide = mm(hi, head_spread) + mm(mid, head_spread) + mm(low, head_spread)
        acc = jnp.exp(last_wide[0:1, :]) * acc_ref[...] + state
        acc_ref[...] = acc
        group = carry_ref[0:1, :]
        pair = jnp.where(j == 2, 0.0, carry_ref[1:2, :])
        e2_ref[j] = jnp.exp(cum + pair)
        lane = lax.broadcasted_iota(jnp.int32, (128, 128), 1)
        src = lax.broadcasted_iota(jnp.int32, (128, 128), 0)
        to_levels = jnp.where(src - HEADS * 8 == lane // 8, 1.0, 0.0)
        sc_ref[j] = (sp * mm(jnp.exp(cum + group), to_levels)).astype(BF)
        carry_ref[0:1, :] = group + last
        carry_ref[1:2, :] = pair + last
        xs_ref[j] = xs
        b_ref[j] = b_mat.astype(BF)
        sp_ref[j] = sp
        cum_ref[j] = cum
        row_ref[j] = cum.T[HEADS * 8 : HEADS * 9, :]
        s_ref[j] = state.astype(BF)
        logs_ref[0:1, :] = logs_ref[0:1, :] + last_wide[0:1, :]

        @pl.when(j == 1)
        def _():
            pair_ref[...] = acc.astype(BF)

        @pl.when(j == NY - 1)
        def _():
            pack_message(msg_ref, acc, logs_ref[0:1, :])

    each_block(block)


def pack_message(msg_ref, state, log):
    msg_ref[0:NS, :] = state.astype(BF)
    hi = log.astype(BF).astype(F32)
    row = lax.broadcasted_iota(jnp.int32, (16, XW), 0)
    both = jnp.where(row == 0, hi, jnp.where(row == 1, log - hi, 0.0))
    msg_ref[NS:, :] = both.astype(BF)


def run_state(part, rows, far_a, far_b, taps, bias, small_bias, rate, spreads):
    return run(
        state_kernel,
        (),
        (part, rows, far_a, far_b, taps, bias, small_bias, rate, spreads),
        [
            plain(F32, NY, ROWS, XW), plain(BF, NY, ROWS, NS), plain(F32, NY, ROWS, 128),
            plain(F32, NY, ROWS, 128), plain(F32, NY, ROWS, 128), plain(BF, NY, ROWS, 128),
            plain(F32, NY, HEADS, ROWS), plain(BF, NY, NS, XW),
            plain(BF, NS, XW), shape_of(F32, 16, XW), shape_of(BF, NS + 16, XW),
        ],
        [
            pltpu.VMEM((EXT, XW + NS), F32),
            pltpu.VMEM((NS, XW), F32),
            pltpu.VMEM((8, 128), F32),
        ],
    )


def intra_kernel(
    part_ref, rows_ref, far_ref, taps_ref, bias_ref, skip_ref,
    xs_ref, b_ref, sp_ref, cum_ref, e2_ref, row_ref, s1_ref, s2_ref, spread_ref,
    y_ref, c_ref, z_ref, wide_ref, *, base,
):
    j = pl.program_id(0) + base
    p = part_ref[0] + jnp.dot(rows_ref[0], far_ref[...], preferred_element_type=F32)
    p = p.astype(BF).astype(F32)
    z_ref[0] = p[HALO:, :XW].astype(BF)
    wide_ref[...] = p[:, XW:]
    c_mat = conv_block(wide_ref, taps_ref, bias_ref).astype(BF)
    c_ref[0] = c_mat
    xs = xs_ref[0]
    sp = sp_ref[0].astype(BF)
    cum = cum_ref[0]
    scores = lax.dot_general(
        c_mat, b_ref[0], (((1,), (1,)), ((), ())), preferred_element_type=F32
    )
    row = lax.broadcasted_iota(jnp.int32, (ROWS, ROWS), 0)
    col = lax.broadcasted_iota(jnp.int32, (ROWS, ROWS), 1)
    causal = col <= row
    head_spread = spread_ref[8]
    xd = (xs * mm(sp, head_spread)).astype(BF)
    parts = []
    for h in range(HEADS):
        lane = HEADS * 8 + h
        halves = []
        for top, width in ((0, ROWS // 2), (ROWS // 2, ROWS)):
            here = slice(top, top + ROWS // 2)
            diff = cum[here, lane : lane + 1] - row_ref[0, h : h + 1, :width]
            decay = jnp.exp(jnp.where(causal[here, :width], diff, -1e30)) * scores[here, :width]
            halves.append(mm(decay, xd[:width, h * HD : (h + 1) * HD]))
        parts.append(jnp.concatenate(halves, axis=0))
    y = jnp.concatenate(parts, axis=1) * mm(sp, spread_ref[0])
    y = y + skip_ref[0:1, :] * xs
    odd = (j % 2).astype(F32)
    late = (j // 2).astype(F32)
    one = mm(sp, spread_ref[1]) * mm(jnp.exp(cum), head_spread)
    y = y + mm(c_mat, s1_ref[0]) * (one * odd)
    two = mm(sp, spread_ref[2]) * mm(e2_ref[0], head_spread)
    y = y + mm(c_mat, s2_ref[...]) * (two * late)
    y_ref[0] = y


def run_intra(base, part, rows, w_far, taps, bias, skip, xs, b_mat, sp, cum, e2, row, states, pair, spreads):
    whole = lambda *shape: pl.BlockSpec(shape, lambda j: (0,) * len(shape))
    each = lambda a, b: pl.BlockSpec((1, a, b), lambda j: (j + base, 0, 0))
    own = lambda a, b: pl.BlockSpec((1, a, b), lambda j: (j, 0, 0))
    arrays = (part, rows, w_far, taps, bias, skip, xs, b_mat, sp, cum, e2, row, states, pair, spreads)
    arrays = [v.value if isinstance(v, Kept) else far(v) for v in arrays]
    half = NY // 2
    outs = [plain(F32, half, ROWS, XW), plain(BF, half, ROWS, NS), plain(BF, half, ROWS, XW)]
    results = pl.pallas_call(
        functools.partial(intra_kernel, base=base),
        grid=(half,),
        in_specs=[
            each(EXT, WB), each(EXT, KX), whole(KX, WB),
            whole(4, NS), whole(1, NS), whole(1, XW),
            each(ROWS, XW), each(ROWS, NS), each(ROWS, 128), each(ROWS, 128), each(ROWS, 128),
            each(HEADS, ROWS),
            pl.BlockSpec((1, NS, XW), lambda j: (base, 0, 0)),
            whole(NS, XW), whole(9, 128, XW),
        ],
        out_specs=[own(ROWS, XW), own(ROWS, NS), own(ROWS, XW)],
        out_shape=outs,
        scratch_shapes=[pltpu.VMEM((EXT, NS), F32)],
        compiler_params=pltpu.CompilerParams(vmem_limit_bytes=28 << 20),
        name="intra_block",
    )(*arrays)
    return [Kept(v, out) for v, out in zip(results, outs, strict=True)]


def merge_kernel(mask_ref, got_ref, own_ref, logs_ref, msg_ref, new_logs_ref, *, k):
    upper = mask_ref[k : k + 1, :] == 1
    other = got_ref[0:NS, :].astype(F32)
    tail = got_ref[NS:, :].astype(F32)
    other_log = tail[0:1, :] + tail[1:2, :]
    log = logs_ref[0:1, :]
    before = logs_ref[1:2, :]
    state = (
        jnp.where(upper, jnp.exp(log), 1.0) * other
        + jnp.where(upper, 1.0, jnp.exp(other_log)) * own_ref[0:NS, :].astype(F32)
    )
    log = log + other_log
    new_logs_ref[...] = logs_ref[...]
    new_logs_ref[0:1, :] = log
    new_logs_ref[1:2, :] = jnp.where(upper, before + other_log, before)
    new_logs_ref[8 + k : 9 + k, :] = jnp.where(upper, jnp.exp(before), 0.0)
    pack_message(msg_ref, state, log)


def run_merge(k, masks, got, own, logs):
    return run(
        functools.partial(merge_kernel, k=k),
        (),
        (masks, got, own, logs),
        [shape_of(BF, NS + 16, XW), shape_of(F32, 16, XW)],
    )


def cross_kernel(
    at_ref, ya_ref, ca_ref, za_ref, yb_ref, cb_ref, zb_ref, sc_ref, g3, g4, g5, g6, g7, logs_ref, spread_ref,
    q0, q1, q2, q3, bucket_ref,
):
    for k, got in enumerate((g3, g4, g5, g6, g7)):
        scaled = got[0:NS, :].astype(F32) * logs_ref[8 + k : 9 + k, :]
        bucket_ref[k] = scaled.astype(BF)
    for k, q_ref in enumerate((q0, q1, q2, q3)):
        j = (at_ref[0] + k) % NY
        first = j < NY // 2
        near_j = j % (NY // 2)
        c_mat = jnp.where(first, ca_ref[near_j], cb_ref[near_j])
        scale = sc_ref[j]
        y = jnp.where(first, ya_ref[near_j], yb_ref[near_j])
        gate = jnp.where(first, za_ref[near_j], zb_ref[near_j]).astype(F32)
        for level in range(3, 8):
            y = y + mm(c_mat, bucket_ref[level - 3]) * mm(scale, spread_ref[level])
        q_ref[...] = (y * silu(gate)).astype(BF)


def run_cross(at, inner, sc, gots, logs, spreads):
    return run(
        cross_kernel,
        (at,),
        (*inner, sc, *gots, logs, spreads),
        [shape_of(BF, ROWS, XW)] * NY,
        [pltpu.VMEM((5, NS, XW), BF)],
        place=lambda v: v,
    )


def out_kernel(at_ref, q0, q1, q2, q3, gain_ref, acts_ref, w_ref, out_ref, acc_ref, w_vmem, sems):
    blocks = (q0, q1, q2, q3)
    rows = [
        pl.ds(pl.multiple_of(((at_ref[0] + NY - k) % NY) * XW, XW), XW) for k in range(NY)
    ]
    copies = [
        pltpu.make_async_copy(w_ref.at[rows[k], :], w_vmem.at[k], sems.at[k]) for k in range(NY)
    ]
    for copy in copies:
        copy.start()
    square = sum(
        jnp.sum(jnp.square(q[...].astype(F32)), axis=1, keepdims=True) for q in blocks
    )
    scale = lax.rsqrt(square / (NY * XW) + EPS)
    acc_ref[...] = acts_ref[...].astype(F32)
    for k, q in enumerate(blocks):
        n = q[...].astype(F32) * scale * gain_ref[0:1, rows[k]]
        copies[k].wait()
        acc_ref[...] += jnp.dot(n.astype(BF), w_vmem[k], preferred_element_type=F32)
    out_ref[...] = acc_ref[...].astype(BF)


def run_out(at, blocks, gain, weight, acts):
    width = weight.shape[1]
    vmem = pl.BlockSpec(memory_space=pltpu.VMEM)
    blocks = [v.value if isinstance(v, Kept) else near(v) for v in blocks]
    return pl.pallas_call(
        out_kernel,
        in_specs=[pl.BlockSpec(memory_space=pltpu.SMEM)]
        + [vmem] * 6
        + [pl.BlockSpec(memory_space=pltpu.HBM)],
        out_specs=vmem,
        out_shape=shape_of(BF, ROWS, width),
        scratch_shapes=[
            pltpu.VMEM((ROWS, width), F32),
            pltpu.VMEM((NY, XW, width), BF),
            pltpu.SemaphoreType.DMA((NY,)),
        ],
        compiler_params=pltpu.CompilerParams(vmem_limit_bytes=28 << 20),
        name="gate_out",
    )(at, *blocks, gain, acts, far(weight))


def norm_kernel(at_ref, halo_ref, acts_ref, gain_ref, out_ref, full_ref):
    for start, ref in ((0, halo_ref), (HALO, acts_ref)):
        v = ref[...].astype(F32)
        scale = lax.rsqrt(jnp.mean(v * v, axis=1, keepdims=True) + EPS)
        full_ref[start : start + v.shape[0], :] = v * scale * gain_ref[0:1, :]
    for k in range(NX):
        start = pl.multiple_of(at_ref[1 + k] * KX, KX)
        part = pltpu.roll(full_ref[:, pl.ds(start, KX)], at_ref[1 + NX], 1)
        out_ref[:, k * KX : (k + 1) * KX] = part.astype(BF)


def run_norm(at, halo, acts, gain):
    width = acts.shape[1]
    return run(
        norm_kernel,
        (at,),
        (halo, acts, gain),
        [shape_of(BF, EXT, width)],
        [pltpu.VMEM((EXT, width), F32)],
        place=far,
    )[0]


def columns_kernel(y_ref, shard_ref, o0, o1, o2, o3, all_ref):
    shard = shard_ref[...]
    for t in range(NY):
        x0, z0 = t * XW, 2304 + t * XW
        dt0, lv0 = 4352 + t * HEADS, 4384 + t * HEADS * 8
        all_ref[t, :, 0:XW] = shard[:, x0 : x0 + XW]
        all_ref[t, :, XW : XW + NS] = shard[:, 2048 : 2048 + NS]
        all_ref[t, :, XW + NS : WA] = jnp.concatenate(
            [
                shard[:, lv0 : lv0 + HEADS * 8].astype(F32),
                shard[:, dt0 : dt0 + HEADS].astype(F32),
                jnp.zeros((shard.shape[0], 128 - HEADS * 9), F32),
            ],
            axis=1,
        ).astype(BF)
        all_ref[t, :, WA : WA + XW] = shard[:, z0 : z0 + XW]
        all_ref[t, :, WA + XW :] = shard[:, 2048 + NS : 2304]
    for k, out in enumerate((o0, o1, o2, o3)):
        out[...] = all_ref[(y_ref[0] + k) % NY]


def run_columns(y, shard):
    rows = shard.shape[0]
    return run(
        columns_kernel,
        (y,),
        (shard,),
        [shape_of(BF, rows, WA + WB)] * 4,
        [pltpu.VMEM((NY, rows, WA + WB), BF)],
        place=lambda v: v,
    )


def join_kernel(y_ref, b0, b1, b2, b3, out_ref):
    rows = b0.shape[0]
    for back, block in ((0, b0), (3, b1), (2, b2), (1, b3)):
        start = pl.multiple_of(((y_ref[0] + back) % NY) * rows, rows)
        out_ref[pl.ds(start, rows), :] = block[...]


def run_join(y, blocks):
    rows, width = blocks[0].shape
    return run(join_kernel, (y,), blocks, [shape_of(BF, NY * rows, width)])[0]


def gather_kernel(*refs):
    *blocks, a_ref, b_ref = refs
    rows = blocks[0].shape[0]
    for k, block in enumerate(blocks):
        a_ref[k * rows : (k + 1) * rows, :] = block[:, :WA]
        b_ref[k * rows : (k + 1) * rows, :] = block[:, WA:]


def together(*values):
    return lax.optimization_barrier(values)


def ring_z(block):
    up, down = [block], [block]
    for k in range(4):
        up.append(sent(up[-1], Z_UP))
        if k < 3:
            down.append(sent(down[-1], Z_DOWN))
    return down + [up[4], up[3], up[2], up[1]]


def half_kernel(block_ref, out_ref, *, start):
    out_ref[...] = block_ref[start : start + out_ref.shape[0], :]


def rows_from(block, start, count):
    kernel = functools.partial(half_kernel, start=start)
    return run(kernel, (), (block,), [shape_of(BF, count, block.shape[1])])[0]


def near_pair(block, up, down):
    return sent(block, up), sent(block, down)


def far_pair(below, above, up, down, split):
    rest = above.shape[0] - split
    return sent(rows_from(below, 0, split), up), sent(rows_from(above, split, rest), down)


def mask_kernel(bits_ref, out_ref):
    for k in range(5):
        out_ref[k : k + 1, :] = jnp.full((1, XW), bits_ref[2 + NX + k], jnp.int32)


def layer(
    acts,
    in_proj,
    out_proj,
    conv_weight,
    conv_bias,
    dt_bias,
    decay_rate,
    skip_gain,
    level_bias,
    norm_gain,
    gate_gain,
):
    index = lax.axis_index("seq")
    y = index % NY
    z = (index // NY) % NZ
    x = index // (NY * NZ)
    bits = [z & 1, (z >> 1) & 1, (z >> 2) & 1, x & 1, (x >> 1) & 1]
    where = jnp.stack(
        [y, x, (x + 3) % NX, (x + 1) % NX, (x + 2) % NX, (512 - 64 * z) % 512, *bits]
    )
    w0, w1, w2, w3 = run_columns(where, in_proj[0])
    shared = (w0, sent(w1, Y_UP), sent(w2, Y_TWO), sent(w3, Y_DOWN))
    columns = run_join(where, shared)
    halo = sent(acts[0, ROWS - HALO :], HALO_NEXT)
    u = run_norm(where, halo, acts[0], norm_gain)

    blocks = ring_z(columns)
    below, above = near_pair(u, Y_UP, Y_DOWN)
    far_lo, far_hi = far_pair(below, above, Y_UP, Y_DOWN, SPLIT)
    rows, rows_far = run(
        stack_kernel, (where,), (u, below, above, far_lo, far_hi),
        [plain(BF, NY, EXT, 3 * KX), plain(BF, NY, EXT, KX)],
    )
    depth = len(blocks) * blocks[1].shape[0]
    by_a, by_b = run(gather_kernel, (), blocks, [shape_of(BF, depth, WA), plain(BF, depth, WB)])

    y, _ = together(y, blocks[7])
    piece = lambda v, width: lax.dynamic_slice_in_dim(v, y * width, width, v.ndim - 1)
    taps_a = jnp.concatenate(
        [piece(conv_weight[0, :, :2048], XW), conv_weight[0, :, 2048 : 2048 + NS]], axis=1
    )
    bias_a = jnp.concatenate(
        [piece(conv_bias[:, :2048], XW), conv_bias[:, 2048 : 2048 + NS]], axis=1
    )
    pad = jnp.zeros((1, 128 - HEADS * 9), F32)
    small_bias = jnp.concatenate(
        [piece(level_bias, HEADS * 8), piece(dt_bias, HEADS), pad], axis=1
    )
    rate = jnp.concatenate(
        [jnp.zeros((1, HEADS * 8), F32), piece(decay_rate, HEADS), pad], axis=1
    )
    skip = jnp.repeat(piece(skip_gain, HEADS), HD, axis=1)
    spreads = run(spread_kernel, (), (), [plain(BF, 9, 128, XW)])[0]
    masks = run(mask_kernel, (where,), (), [shape_of(jnp.int32, 8, XW)])[0]

    a_below, a_above = near_pair(by_a, X_UP, X_DOWN)
    fa_a, fb_a = far_pair(a_below, a_above, X_UP, X_DOWN, KX // 2)
    part_a = run_part(rows, by_a, a_below, a_above, shape_of)

    b_below, b_above = near_pair(by_b, X_UP, X_DOWN)
    w_far = sent(by_b, X_TWO)
    xs, b_mat, sp, cum, e2, sc, row, states, pair, logs, message = run_state(
        part_a, rows_far, fa_a, fb_a, taps_a, bias_a, small_bias, rate, spreads
    )
    part_b = run_part(rows, by_b, b_below, b_above, plain)

    gots = []
    for k, pairs in enumerate(EXCHANGES):
        got = sent(message, pairs)
        message, logs = run_merge(k, masks, got, message, logs)
        gots.append(got)

    inner = []
    for base in (0, NY // 2):
        inner += run_intra(
            base, part_b, rows_far, w_far, conv_weight[0, :, 2048 + NS :], conv_bias[:, 2048 + NS :], skip,
            xs, b_mat, sp, cum, e2, row, states, pair, spreads,
        )
    q0, q1, q2, q3 = run_cross(where, inner, sc, gots, logs, spreads)
    back_two = sent(q2, Y_TWO)
    blocks = (q0, sent(q1, Y_UP), back_two, sent(q3, Y_DOWN))
    result = run_out(where, blocks, gate_gain, out_proj[0], acts[0])
    return lax.ppermute(result, "section", [(0, 1), (1, 0)])[None]


def solution(mesh):
    return jax.shard_map(
        layer,
        mesh=mesh,
        in_specs=(
            P("section", "seq", None),
            P("section", "seq", None),
            P("section", None, None),
            P("section", None, None),
            P("section", None),
            P("section", None),
            P("section", None),
            P("section", None),
            P("section", None),
            P("section", None),
            P("section", None),
        ),
        out_specs=P("section", "seq", None),
        check_vma=False,
    )
```
